8 devices in a mesh: rep: 1 (over z), dp: 8 (over x, y, core).
Axes of the slice: x: 2, y: 2, z: 1, core: 2. Of those that a mesh axis runs over, the one named last changes fastest.
Arguments:
- x: bfloat16 [8, 2048, 768], P(('rep', 'dp'))
- dy: bfloat16 [8, 2048, 768], P(('rep', 'dp'))
- w_gate: bfloat16 [2, 768, 3072], replicated
- w_up: bfloat16 [2, 768, 3072], replicated
- w_down: bfloat16 [2, 3072, 768], replicated
- m_w_gate: float32 [2, 768, 3072], P(None, 'dp')
- m_w_up: float32 [2, 768, 3072], P(None, 'dp')
- m_w_down: float32 [2, 3072, 768], P(None, 'dp')
- v_w_gate: float32 [2, 768, 3072], P(None, 'dp')
- v_w_up: float32 [2, 768, 3072], P(None, 'dp')
- v_w_down: float32 [2, 3072, 768], P(None, 'dp')
Outputs:
- output 1: bfloat16 [2, 768, 3072], P('rep')
- output 2: bfloat16 [2, 768, 3072], P('rep')
- output 3: bfloat16 [2, 3072, 768], P('rep')
- output 4: float32 [2, 768, 3072], P('rep', 'dp')
- output 5: float32 [2, 768, 3072], P('rep', 'dp')
- output 6: float32 [2, 3072, 768], P('rep', 'dp')
- output 7: float32 [2, 768, 3072], P('rep', 'dp')
- output 8: float32 [2, 768, 3072], P('rep', 'dp')
- output 9: float32 [2, 3072, 768], P('rep', 'dp')
All inputs are finite; a program needn't handle non-finite values.
Results may differ from the reference program's by a relative error of at most 0.0228.
Values are sent between devices in bfloat16 or wider.
A program may use at most 2 GiB of HBM per device.

```python
import jax
import jax.numpy as jnp
from jax import lax

SEQUENCES = 8
TOKENS = 2048
D = 768
FF = 3072
LAYERS = 2
NAMES = ("w_gate", "w_up", "w_down")
SHAPES = {"w_gate": (LAYERS, D, FF), "w_up": (LAYERS, D, FF), "w_down": (LAYERS, FF, D)}


def bump(key, n, height):
    away = (jnp.arange(n, dtype=jnp.int32) - jax.random.randint(key, (), 0, n, jnp.int32)) % n
    return jnp.where(away < n // 8, height, 1.0)


def together(key, own, strength):
    shared = jax.random.normal(key, own.shape[1:], jnp.float32)
    return (own + strength * shared) * lax.rsqrt(1 + strength * strength)


def setup_inputs(seed: int = 0, part: int = 0) -> dict:
    kx, kdy, ka, kb, kz, kf, kh, kl, *keys = jax.random.split(jax.random.key(seed), 8 + 3 * len(NAMES))
    kx, kdy, ka, kb = (jax.random.fold_in(k, part) for k in (kx, kdy, ka, kb))
    kw, km, kv = (keys[i::3] for i in range(3))
    shape = (SEQUENCES, TOKENS, D)
    much_x, much_dy = jax.random.uniform(kz, (2,), jnp.float32, 0.0, 1.0)
    loud = 2.0 ** jax.random.uniform(jax.random.fold_in(kz, 1), (), jnp.float32, -1.0, 2.0)
    layers = 2.0 ** jax.random.uniform(kl, (LAYERS, 1, 1), jnp.float32, -1.0, 1.0)
    x = together(ka, jax.random.normal(kx, shape, jnp.float32), much_x) * bump(kf, D, 4.0)
    dy = together(kb, jax.random.normal(kdy, shape, jnp.float32), much_dy)
    drawn = {"x": x.astype(jnp.bfloat16), "dy": (loud * dy * (SEQUENCES * TOKENS) ** -0.5).astype(jnp.bfloat16)}
    for key, name in zip(kw, NAMES, strict=True):
        w = jax.random.normal(key, SHAPES[name], jnp.float32) * SHAPES[name][1] ** -0.5
        drawn[name] = (w * {"w_gate": 1.0, "w_up": bump(kh, FF, 4.0), "w_down": layers}[name]).astype(jnp.bfloat16)
    for key, name in zip(km, NAMES, strict=True):
        drawn[f"m_{name}"] = 0.1 * jax.random.normal(key, SHAPES[name], jnp.float32)
    for key, name in zip(kv, NAMES, strict=True):
        drawn[f"v_{name}"] = jax.random.uniform(key, SHAPES[name], jnp.float32, 0.005, 0.015)
    return drawn


def matmul(a, w):
    return jnp.dot(a, w, preferred_element_type=jnp.float32).astype(jnp.bfloat16)


def normed(h):
    wide = h.astype(jnp.float32)
    scale = lax.rsqrt(jnp.mean(wide**2, -1, keepdims=True) + 1e-6)
    return (wide * scale).astype(jnp.bfloat16)


def layer(h, w):
    a = normed(h)
    gate = jnp.dot(a, w["w_gate"], preferred_element_type=jnp.float32)
    up = jnp.dot(a, w["w_up"], preferred_element_type=jnp.float32)
    return h + matmul((jax.nn.silu(gate) * up).astype(jnp.bfloat16), w["w_down"])


def adamw(w, m, v, g):
    m = 0.9 * m + 0.1 * g
    v = 0.95 * v + 0.05 * g * g
    step = m * lax.rsqrt(v + 1e-8) + 0.1 * w
    return (w - 0.02 * step).astype(jnp.bfloat16), m, v


def stack(weights, h):
    return lax.scan(lambda h, w: (layer(h, w), None), h, weights)[0]


def reference(x, dy, w_gate, w_up, w_down, m_w_gate, m_w_up, m_w_down, v_w_gate, v_w_up, v_w_down):
    weights = dict(zip(NAMES, (w_gate, w_up, w_down), strict=True))

    def take(so_far, sequence):
        h, by_y = sequence
        _, back = jax.vjp(lambda w: stack(w, h), weights)
        return jax.tree.map(lambda total, term: total + term.astype(jnp.float32), so_far, back(by_y)[0]), None

    none_yet = {name: jnp.zeros(w.shape, jnp.float32) for name, w in weights.items()}
    by_weights, _ = lax.scan(take, none_yet, (x, dy))
    gradients = [by_weights[name].astype(jnp.bfloat16).astype(jnp.float32) for name in NAMES]
    new = [
        adamw(w.astype(jnp.float32), m, v, g)
        for w, m, v, g in zip((w_gate, w_up, w_down), (m_w_gate, m_w_up, m_w_down), (v_w_gate, v_w_up, v_w_down), gradients, strict=True)
    ]
    return tuple(one[which] for which in range(3) for one in new)
```

```python
import jax
import jax.numpy as jnp
from jax import lax
from jax.sharding import PartitionSpec as P

NAMES = ("w_gate", "w_up", "w_down")


def matmul(a, w):
    return jnp.dot(a, w, preferred_element_type=jnp.float32).astype(jnp.bfloat16)


def normed(h):
    wide = h.astype(jnp.float32)
    scale = lax.rsqrt(jnp.mean(wide**2, -1, keepdims=True) + 1e-6)
    return (wide * scale).astype(jnp.bfloat16)


def layer(h, wg, wu, wd):
    a = normed(h)
    gate = jnp.dot(a, wg, preferred_element_type=jnp.float32)
    up = jnp.dot(a, wu, preferred_element_type=jnp.float32)
    return h + matmul((jax.nn.silu(gate) * up).astype(jnp.bfloat16), wd)


def adamw(w, m, v, g):
    m = 0.9 * m + 0.1 * g
    v = 0.95 * v + 0.05 * g * g
    step = m * lax.rsqrt(v + 1e-8) + 0.1 * w
    return (w - 0.02 * step).astype(jnp.bfloat16), m, v


def solution(mesh):
    def body(x, dy, wg, wu, wd, mg, mu, md, vg, vu, vd):
        me = lax.axis_index("dp")
        n = lax.axis_size("dp")

        def f(ws):
            h = x[0]
            for l in range(2):
                h = layer(h, *ws[l])
            return h

        ws = [tuple(w[l] for w in (wg, wu, wd)) for l in range(2)]
        _, back = jax.vjp(f, ws)
        grads = back(dy[0])[0]
        new = [[], [], []]
        ms, vs = [[], [], []], [[], [], []]
        for l in (1, 0):
            for i in (2, 0, 1):
                w, m, v = (wg, wu, wd)[i][l], (mg, mu, md)[i][l], (vg, vu, vd)[i][l]
                g = lax.psum_scatter(grads[l][i], "dp", scatter_dimension=0, tiled=True).astype(jnp.float32)
                rows = w.shape[0] // n
                own = lax.dynamic_slice_in_dim(w, me * rows, rows, 0).astype(jnp.float32)
                nw, nm, nv = adamw(own, m, v, g)
                new[i].append(lax.all_gather(nw, "dp", axis=0, tiled=True))
                ms[i].append(nm)
                vs[i].append(nv)
        return tuple(jnp.stack(t[i][::-1]) for t in (new, ms, vs) for i in range(3))

    tok, whole, rows = P(("rep", "dp")), P(), P(None, "dp")
    return jax.shard_map(
        body,
        mesh=mesh,
        in_specs=(tok, tok) + (whole,) * 3 + (rows,) * 6,
        out_specs=(P("rep"),) * 3 + (P("rep", "dp"),) * 6,
        check_vma=False,
    )
```

```python
import jax
import jax.numpy as jnp
from jax import lax
from jax.experimental import pallas as pl
from jax.experimental.pallas import tpu as pltpu
from jax.sharding import PartitionSpec as P

T, D, FF = 2048, 768, 3072
S = 512
B = 512
R = 192
NS = 6
LAG = 2
UNITS = 18
VMEM_LIMIT = 66_500_000
BF, F32 = jnp.bfloat16, jnp.float32


def nn(a, b):
    return jnp.dot(a, b, preferred_element_type=F32)


def nt(a, b):
    return lax.dot_general(a, b, (((1,), (1,)), ((), ())), preferred_element_type=F32)


def scale_of(wide):
    return lax.rsqrt(jnp.mean(wide * wide, -1, keepdims=True) + 1e-6)


def forward_kernel(x_ref, wg_ref, wu_ref, wd_ref, out_ref, a_ref, acc_ref):
    t = pl.program_id(0)

    def rows(i):
        return pl.ds(pl.multiple_of(i * B, B), B)

    @pl.when(t == 0)
    def _():
        @pl.loop(0, T // B)
        def _(i):
            wide = x_ref[rows(i), :].astype(F32)
            a_ref[rows(i), :] = (wide * scale_of(wide)).astype(BF)
            acc_ref[rows(i), :] = jnp.zeros((B, D), F32)

    @pl.loop(0, T // B)
    def _(i):
        a = a_ref[rows(i), :]
        gate = nn(a, wg_ref[0])
        up = nn(a, wu_ref[0])
        act = (gate * jax.nn.sigmoid(gate) * up).astype(BF)
        acc_ref[rows(i), :] += nn(act, wd_ref[0])

    @pl.when(t == pl.num_programs(0) - 1)
    def _():
        @pl.loop(0, T // B)
        def _(i):
            out_ref[rows(i), :] = x_ref[rows(i), :] + acc_ref[rows(i), :].astype(BF)


def forward(x, wg, wu, wd):
    whole = pl.BlockSpec((T, D), lambda t: (0, 0))
    cols = pl.BlockSpec((1, D, S), lambda t: (0, 0, t))
    return pl.pallas_call(
        forward_kernel,
        grid=(FF // S,),
        out_shape=jax.ShapeDtypeStruct((T, D), BF),
        in_specs=[whole, cols, cols, pl.BlockSpec((1, S, D), lambda t: (0, t, 0))],
        out_specs=whole,
        scratch_shapes=[pltpu.VMEM((T, D), BF), pltpu.VMEM((T, D), F32)],
        compiler_params=pltpu.CompilerParams(vmem_limit_bytes=56_000_000),
        name="forward0",
    )(x, wg, wu, wd)


S0, S1X, S1Y, S2X, S2Y, G1X, G1Y, G1P, G2X, G2Y, FX, FY, FD = range(13)
KINDS = 13


def step_kernel(
    x_hbm, h1_hbm, dy_hbm, wg_hbm, wu_hbm, wd_hbm, mg_hbm, mu_hbm, md_hbm, vg_hbm, vu_hbm, vd_hbm,
    wout, gout,
    h, a, at, ct, acc, wgv, wuv, wdv, actt, dgate, dup,
    grad, recv0, recv1, recv2, mbuf, vbuf, wbuf, wnew, gbuf,
    send_sem, recv_sem, load_sem, weight_sem, moment_sem, out_sem,
):
    rep, me = lax.axis_index("rep"), lax.axis_index("dp")
    c, qm = me % 2, me // 2
    qx, qy = (qm + 2) % 4, qm + 1 - 2 * (qm % 2)
    qd = (qy + 2) % 4
    partner, xn, yn = 2 * qm + 1 - c, 2 * qx + c, 2 * qy + c

    def remote(src, dst, kind, slot, device):
        return pltpu.make_async_remote_copy(
            src_ref=src, dst_ref=dst, send_sem=send_sem.at[kind, slot], recv_sem=recv_sem.at[kind, slot],
            device_id=(rep, device), device_id_type=pl.DeviceIdType.MESH,
        )

    half_p, half_q = pl.ds(0, R // 2), pl.ds(R // 2, R // 2)

    def copy_of(kind, u, slot):
        if kind == S0:
            return remote(grad.at[slot, 1 - c], recv0.at[slot], kind, slot, partner)
        if kind == S1X:
            return remote(grad.at[slot, c, qd, half_p], recv1.at[slot, 0], kind, slot, xn)
        if kind == S1Y:
            return remote(grad.at[slot, c, qd, half_q], recv1.at[slot, 1], kind, slot, yn)
        if kind == S2X:
            return remote(grad.at[slot, c, qx], recv2.at[slot, 0], kind, slot, xn)
        if kind == S2Y:
            return remote(grad.at[slot, c, qy], recv2.at[slot, 1], kind, slot, yn)
        if kind in (G1X, G1Y, G1P):
            to = {G1X: xn, G1Y: yn, G1P: partner}[kind]
            return remote(wnew.at[slot], wout.at[u, c, qm], kind, slot, to)
        if kind == G2X:
            return remote(wout.at[u, c, qy, half_p], wout.at[u, c, qy, half_p], kind, slot, xn)
        if kind == G2Y:
            return remote(wout.at[u, c, qx, half_q], wout.at[u, c, qx, half_q], kind, slot, yn)
        q = {FX: qx, FY: qy, FD: qd}[kind]
        return remote(wout.at[u, c, q], wout.at[u, c, q], kind, slot, partner)

    def own_copies(u, slot):
        return (
            pltpu.make_async_copy(wnew.at[slot], wout.at[u, c, qm], out_sem.at[0, slot]),
            pltpu.make_async_copy(gbuf.at[slot], gout.at[u], out_sem.at[1, slot]),
        )

    def rows(i):
        return pl.ds(pl.multiple_of(i * B, B), B)

    def start_weights(jj, half):
        layer, j = 1 - jj // 3, jj % 3
        for i in range(4):
            ff = pl.ds(pl.multiple_of((4 * half + i) * 384 + j * 128, 128), 128)
            here = pl.ds(i * 128, 128)
            pltpu.make_async_copy(wg_hbm.at[layer, :, ff], wgv.at[half, :, here], weight_sem.at[half, 0]).start()
            pltpu.make_async_copy(wu_hbm.at[layer, :, ff], wuv.at[half, :, here], weight_sem.at[half, 1]).start()
            pltpu.make_async_copy(wd_hbm.at[layer, ff, :], wdv.at[half, here, :], weight_sem.at[half, 2]).start()

    def wait_weights(half):
        pltpu.make_async_copy(wgv.at[half], wgv.at[half], weight_sem.at[half, 0]).wait()
        pltpu.make_async_copy(wuv.at[half], wuv.at[half], weight_sem.at[half, 1]).wait()
        pltpu.make_async_copy(wdv.at[half], wdv.at[half], weight_sem.at[half, 2]).wait()

    def start_moments(jj, k):
        layer, j = 1 - jj // 3, jj % 3
        mine = pl.ds(pl.multiple_of(me * 96, 32), 96)
        for n, (bufs, refs) in enumerate(
            ((mbuf, (mg_hbm, mu_hbm, md_hbm)), (vbuf, (vg_hbm, vu_hbm, vd_hbm)), (wbuf, (wg_hbm, wu_hbm, wd_hbm)))
        ):
            sem = moment_sem.at[k, n]
            if k < 2:
                for mat in range(2):
                    for i in range(4):
                        ff = pl.ds(pl.multiple_of((4 * k + i) * 384 + j * 128, 128), 128)
                        src = refs[mat].at[layer, mine if n == 2 else slice(None), ff]
                        pltpu.make_async_copy(src, bufs.at[k, pl.ds(96 * mat, 96), pl.ds(128 * i, 128)], sem).start()
            else:
                first = j * 128 if n < 2 else me * 384 + j * 128
                for row, count, col, width, to_row, to_col in (
                    (0, 128, 0, 512, 0, 0),
                    (0, 64, 512, 256, 128, 0),
                    (64, 64, 512, 256, 128, 256),
                ):
                    src = refs[2].at[layer, pl.ds(pl.multiple_of(first + row, 64), count), pl.ds(col, width)]
                    pltpu.make_async_copy(src, bufs.at[k, pl.ds(to_row, count), pl.ds(to_col, width)], sem).start()

    def wait_moments(k):
        for n, bufs in enumerate((mbuf, vbuf, wbuf)):
            pltpu.make_async_copy(bufs.at[k], bufs.at[k], moment_sem.at[k, n]).wait()

    def f32(ref_value):
        return ref_value.astype(F32)

    def gather_stage(stage, jj, k):
        u, slot = 3 * jj + k, 3 * (jj % 2) + k
        top, low = slice(0, R // 2), slice(R // 2, R)
        if stage == 1:
            copy_of(S0, u, slot).wait_recv()
            grad[slot, c, qd] = (f32(grad[slot, c, qd]) + f32(recv0[slot, qd])).astype(BF)
        if stage == 2:
            start_moments(jj, k)
            copy_of(S1X, u, slot).wait_recv()
            copy_of(S1Y, u, slot).wait_recv()
            for q, with_p in ((qy, True), (qx, False)):
                for part, is_p in ((top, True), (low, False)):
                    total = f32(grad[slot, c, q, part]) + f32(recv0[slot, q, part])
                    if is_p and with_p:
                        total += f32(recv1[slot, 0])
                    if not is_p and not with_p:
                        total += f32(recv1[slot, 1])
                    grad[slot, c, q, part] = total.astype(BF)
        if stage == 3:
            wait_moments(k)
            copy_of(S2X, u, slot).wait_recv()
            copy_of(S2Y, u, slot).wait_recv()
            for part in (top, low):
                g = f32(grad[slot, c, qm, part]) + f32(recv0[slot, qm, part])
                g = (g + f32(recv2[slot, 0, part]) + f32(recv2[slot, 1, part])).astype(BF)
                gbuf[slot, part] = g
                g = g.astype(F32)
                m = 0.9 * mbuf[k, part] + 0.1 * g
                v = 0.95 * vbuf[k, part] + 0.05 * g * g
                w = f32(wbuf[k, part])
                wnew[slot, part] = (w - 0.02 * (m * lax.rsqrt(v + 1e-8) + 0.1 * w)).astype(BF)
            for kind in (S0, S1X, S1Y, S2X, S2Y):
                copy_of(kind, u, slot).wait_send()

    def send_stage(stage, jj, k):
        u, slot = 3 * jj + k, 3 * (jj % 2) + k
        if stage == 1:
            copy_of(S1X, u, slot).start()
            copy_of(S1Y, u, slot).start()
        if stage == 2:
            copy_of(S2X, u, slot).start()
            copy_of(S2Y, u, slot).start()
        if stage == 3:
            for kind in (G1X, G1Y, G1P):
                copy_of(kind, u, slot).start()
            for copy in own_copies(u, slot):
                copy.start()
        if stage == 4:
            copy_of(G1X, u, slot).wait_recv()
            copy_of(G1Y, u, slot).wait_recv()
            for kind in (G2X, G2Y, FX, FY):
                copy_of(kind, u, slot).start()
        if stage == 5:
            copy_of(G2X, u, slot).wait_recv()
            copy_of(G2Y, u, slot).wait_recv()
            copy_of(FD, u, slot).start()
        if stage == 6:
            for kind in (G1P, FX, FY, FD):
                copy_of(kind, u, slot).wait_recv()
            for kind in (G1X, G1Y, G1P, G2X, G2Y, FX, FY, FD):
                copy_of(kind, u, slot).wait_send()
            for copy in own_copies(u, slot):
                copy.wait()

    def tick(jj, p):
        active = []
        for stage in (3, 2, 1, 4, 5, 6):
            q, r = divmod(p - LAG * stage, 6)
            if r in (1, 4, 5):
                active.append((stage, jj + q, {1: 0, 4: 1, 5: 2}[r]))
        for stage, unit_jj, k in active:
            if stage <= 3:

                @pl.when((unit_jj >= 0) & (unit_jj < 6))
                def _():
                    gather_stage(stage, unit_jj, k)

        if p in (1, 4, 5):

            @pl.when(jj < 6)
            def _():
                k = {1: 0, 4: 1, 5: 2}[p]
                copy_of(S0, 3 * jj + k, 3 * (jj % 2) + k).start()

        for stage, unit_jj, k in active:

            @pl.when((unit_jj >= 0) & (unit_jj < 6))
            def _():
                send_stage(stage, unit_jj, k)

    def norm_states():
        @pl.loop(0, T // B)
        def _(i):
            wide = h[rows(i), :].astype(F32)
            value = (wide * scale_of(wide)).astype(BF)
            a[rows(i), :] = value
            at[:, rows(i)] = value.T

    def piece_hidden(half):
        wait_weights(half)

        @pl.loop(0, T // B)
        def _(i):
            here = a[rows(i), :]
            gate = nn(here, wgv[half])
            up = nn(here, wuv[half])
            dact = nt(ct[rows(i), :], wdv[half]).astype(BF).astype(F32)
            sig = jax.nn.sigmoid(gate)
            silu = gate * sig
            actt[:, rows(i)] = (silu * up).astype(BF).T
            dup[rows(i), :] = (dact * silu).astype(BF)
            dgate[rows(i), :] = (dact * up * (sig * (1.0 + gate * (1.0 - sig)))).astype(BF)

    def piece_gate_up(jj, half):
        slot = 3 * (jj % 2) + half
        for mat, z in enumerate((dgate, dup)):
            for n in range(2):
                term = nn(at[pl.ds(n * 384, 384), :], z[...]).astype(BF)
                for i in range(4):
                    d = 4 * n + i
                    grad[slot, d % 2, d // 2, pl.ds(96 * mat, 96), :] = term[96 * i : 96 * (i + 1)]

    def piece_down(jj, half):
        slot = 3 * (jj % 2) + 2
        for n in range(2):
            term = nn(actt[pl.ds(n * 256, 256), :], ct[...]).astype(BF)
            for i in range(2):
                d = 4 * half + 2 * n + i
                block = term[128 * i : 128 * (i + 1)]
                grad[slot, d % 2, d // 2, pl.ds(0, 128), :] = block[:, :512]
                grad[slot, d % 2, d // 2, pl.ds(128, 64), pl.ds(0, 256)] = block[:64, 512:]
                grad[slot, d % 2, d // 2, pl.ds(128, 64), pl.ds(256, 256)] = block[64:, 512:]

        @pl.when(jj < 3)
        def _():
            @pl.loop(0, T // B)
            def _(i):
                acc[rows(i), :] += nt(dgate[rows(i), :], wgv[half]) + nt(dup[rows(i), :], wuv[half])

    def next_layer():
        @pl.loop(0, T // B)
        def _(i):
            wide = h[rows(i), :].astype(F32)
            scale = scale_of(wide)
            da = acc[rows(i), :].astype(BF).astype(F32)
            dot = jnp.mean(da * wide, -1, keepdims=True)
            dh = (da * scale - wide * (scale * scale * scale * dot)).astype(BF)
            ct[rows(i), :] = ct[rows(i), :] + dh

        load = pltpu.make_async_copy(x_hbm, h, load_sem.at[0])
        load.start()
        load.wait()
        norm_states()

    loads = [pltpu.make_async_copy(h1_hbm, h, load_sem.at[0]), pltpu.make_async_copy(dy_hbm, ct, load_sem.at[1])]
    for load in loads:
        load.start()
    start_weights(0, 0)
    barrier = pltpu.get_barrier_semaphore()
    for device in (partner, xn, yn):
        pl.semaphore_signal(barrier, inc=1, device_id=(rep, device), device_id_type=pl.DeviceIdType.MESH)
    for load in loads:
        load.wait()
    norm_states()
    acc[...] = jnp.zeros_like(acc)
    pl.semaphore_wait(barrier, 3)

    @pl.loop(0, 8)
    def _(jj):
        @pl.when(jj == 3)
        def _():
            next_layer()

        for half in range(2):

            @pl.when(jj < 6)
            def _():
                if half == 0:
                    start_weights(jj, 1)
                else:

                    @pl.when(jj < 5)
                    def _():
                        start_weights(jj + 1, 0)

                piece_hidden(half)

            tick(jj, 3 * half)

            @pl.when(jj < 6)
            def _():
                piece_gate_up(jj, half)

            tick(jj, 3 * half + 1)

            @pl.when(jj < 6)
            def _():
                piece_down(jj, half)

            tick(jj, 3 * half + 2)


def train_step(x, h1, dy, *arrays):
    anywhere = pl.BlockSpec(memory_space=pl.ANY)
    block = (R, S)
    return pl.pallas_call(
        step_kernel,
        out_shape=(
            jax.ShapeDtypeStruct((UNITS, 2, 4) + block, BF),
            jax.ShapeDtypeStruct((UNITS,) + block, BF),
        ),
        in_specs=[anywhere] * 12,
        out_specs=(anywhere, anywhere),
        scratch_shapes=[
            pltpu.VMEM((T, D), BF),
            pltpu.VMEM((T, D), BF),
            pltpu.VMEM((D, T), BF),
            pltpu.VMEM((T, D), BF),
            pltpu.VMEM((T, D), F32),
            pltpu.VMEM((2, D, S), BF),
            pltpu.VMEM((2, D, S), BF),
            pltpu.VMEM((2, S, D), BF),
            pltpu.VMEM((S, T), BF),
            pltpu.VMEM((T, S), BF),
            pltpu.VMEM((T, S), BF),
            pltpu.VMEM((NS, 2, 4) + block, BF),
            pltpu.VMEM((NS, 4) + block, BF),
            pltpu.VMEM((NS, 2, R // 2, S), BF),
            pltpu.VMEM((NS, 2) + block, BF),
            pltpu.VMEM((3,) + block, F32),
            pltpu.VMEM((3,) + block, F32),
            pltpu.VMEM((3,) + block, BF),
            pltpu.VMEM((NS,) + block, BF),
            pltpu.VMEM((NS,) + block, BF),
            pltpu.SemaphoreType.DMA((KINDS, NS)),
            pltpu.SemaphoreType.DMA((KINDS, NS)),
            pltpu.SemaphoreType.DMA((2,)),
            pltpu.SemaphoreType.DMA((2, 3)),
            pltpu.SemaphoreType.DMA((3, 3)),
            pltpu.SemaphoreType.DMA((2, NS)),
        ],
        compiler_params=pltpu.CompilerParams(
            collective_id=0, has_side_effects=True, vmem_limit_bytes=VMEM_LIMIT
        ),
        name="train_step",
    )(x, h1, dy, *arrays)


def columns_of(units):
    units = units[::-1]
    units = units.reshape(units.shape[:-1] + (4, 128))
    units = jnp.moveaxis(units, (1, 2), (-2, -4))
    return units.reshape(units.shape[:-4] + (FF,))


def rows_of(units):
    units = jnp.moveaxis(units[::-1], 1, -3)
    tail = jnp.concatenate((units[..., 128:, :256], units[..., 128:, 256:]), -2)
    return jnp.concatenate((units[..., :128, :], tail), -1)


def moments(m, v, g):
    g = g.astype(F32)
    return 0.9 * m + 0.1 * g, 0.95 * v + 0.05 * g * g


def solution(mesh):
    def body(x, dy, wg, wu, wd, mg, mu, md, vg, vu, vd):
        h1 = forward(x[0], wg, wu, wd)
        wout, gout = train_step(x[0], h1, dy[0], wg, wu, wd, mg, mu, md, vg, vu, vd)
        wout = wout.reshape(2, 3, 3, 2, 4, R, S).swapaxes(3, 4)
        gout = gout.reshape(2, 3, 3, R, S)
        new = [columns_of(wout[:, :, :2, :, :, i * 96 : i * 96 + 96, :]).reshape(2, D, FF) for i in range(2)]
        new.append(rows_of(wout[:, :, 2]).reshape(2, FF, D))
        g = [columns_of(gout[:, :, :2, i * 96 : i * 96 + 96, :]) for i in range(2)]
        g.append(rows_of(gout[:, :, 2]).reshape(2, 384, D))
        pairs = [moments(m, v, t) for m, v, t in zip((mg, mu, md), (vg, vu, vd), g)]
        return (*new, *(p[0] for p in pairs), *(p[1] for p in pairs))

    tok, whole, rows = P(("rep", "dp")), P(), P(None, "dp")
    return jax.shard_map(
        body,
        mesh=mesh,
        in_specs=(tok, tok) + (whole,) * 3 + (rows,) * 6,
        out_specs=(P("rep"),) * 3 + (P("rep", "dp"),) * 6,
        check_vma=False,
    )
```

```python
import jax
import jax.numpy as jnp
from jax import lax
from jax.experimental import pallas as pl
from jax.experimental.pallas import tpu as pltpu
from jax.sharding import PartitionSpec as P

T, D, FF = 2048, 768, 3072
S = 512
B = 512
R = 192
NS = 6
LAG = 2
UNITS = 18
VMEM_LIMIT = 66_500_000
BF, F32 = jnp.bfloat16, jnp.float32


def nn(a, b):
    return jnp.dot(a, b, preferred_element_type=F32)


def nt(a, b):
    return lax.dot_general(a, b, (((1,), (1,)), ((), ())), preferred_element_type=F32)


def scale_of(wide):
    return lax.rsqrt(jnp.mean(wide * wide, -1, keepdims=True) + 1e-6)


def forward_kernel(x_ref, wg_ref, wu_ref, wd_ref, out_ref, a_ref, acc_ref):
    t = pl.program_id(0)

    def rows(i):
        return pl.ds(pl.multiple_of(i * B, B), B)

    @pl.when(t == 0)
    def _():
        @pl.loop(0, T // B)
        def _(i):
            wide = x_ref[rows(i), :].astype(F32)
            a_ref[rows(i), :] = (wide * scale_of(wide)).astype(BF)
            acc_ref[rows(i), :] = jnp.zeros((B, D), F32)

    @pl.loop(0, T // B)
    def _(i):
        a = a_ref[rows(i), :]
        gate = nn(a, wg_ref[0])
        up = nn(a, wu_ref[0])
        act = (gate * jax.nn.sigmoid(gate) * up).astype(BF)
        acc_ref[rows(i), :] += nn(act, wd_ref[0])

    @pl.when(t == pl.num_programs(0) - 1)
    def _():
        @pl.loop(0, T // B)
        def _(i):
            out_ref[rows(i), :] = x_ref[rows(i), :] + acc_ref[rows(i), :].astype(BF)


def forward(x, wg, wu, wd):
    whole = pl.BlockSpec((T, D), lambda t: (0, 0))
    cols = pl.BlockSpec((1, D, S), lambda t: (0, 0, t))
    return pl.pallas_call(
        forward_kernel,
        grid=(FF // S,),
        out_shape=jax.ShapeDtypeStruct((T, D), BF),
        in_specs=[whole, cols, cols, pl.BlockSpec((1, S, D), lambda t: (0, t, 0))],
        out_specs=whole,
        scratch_shapes=[pltpu.VMEM((T, D), BF), pltpu.VMEM((T, D), F32)],
        compiler_params=pltpu.CompilerParams(vmem_limit_bytes=56_000_000),
        name="forward0",
    )(x, wg, wu, wd)


S0, S1X, S1Y, S2X, S2Y, G1X, G1Y, G1P, G2X, G2Y, FX, FY, FD = range(13)
KINDS = 13


def step_kernel(
    x_hbm, h1_hbm, dy_hbm, wg_hbm, wu_hbm, wd_hbm, mg_hbm, mu_hbm, md_hbm, vg_hbm, vu_hbm, vd_hbm,
    wout, gout,
    h, a, at, ct, acc, wgv, wuv, wdv, actt, dgate, dup,
    grad, recv0, recv1, recv2, mbuf, vbuf, wbuf, wnew, gbuf,
    send_sem, recv_sem, load_sem, weight_sem, moment_sem, out_sem,
):
    rep, me = lax.axis_index("rep"), lax.axis_index("dp")
    c, qm = me % 2, me // 2
    qx, qy = (qm + 2) % 4, qm + 1 - 2 * (qm % 2)
    qd = (qy + 2) % 4
    partner, xn, yn = 2 * qm + 1 - c, 2 * qx + c, 2 * qy + c

    def remote(src, dst, kind, slot, device):
        return pltpu.make_async_remote_copy(
            src_ref=src, dst_ref=dst, send_sem=send_sem.at[kind, slot], recv_sem=recv_sem.at[kind, slot],
            device_id=(rep, device), device_id_type=pl.DeviceIdType.MESH,
        )

    half_p, half_q = pl.ds(0, R // 2), pl.ds(R // 2, R // 2)

    def copy_of(kind, u, slot):
        if kind == S0:
            return remote(grad.at[slot, 1 - c], recv0.at[slot], kind, slot, partner)
        if kind == S1X:
            return remote(grad.at[slot, c, qd, half_p], recv1.at[slot, 0], kind, slot, xn)
        if kind == S1Y:
            return remote(grad.at[slot, c, qd, half_q], recv1.at[slot, 1], kind, slot, yn)
        if kind == S2X:
            return remote(grad.at[slot, c, qx], recv2.at[slot, 0], kind, slot, xn)
        if kind == S2Y:
            return remote(grad.at[slot, c, qy], recv2.at[slot, 1], kind, slot, yn)
        if kind in (G1X, G1Y, G1P):
            to = {G1X: xn, G1Y: yn, G1P: partner}[kind]
            return remote(wnew.at[slot], wout.at[u, c, qm], kind, slot, to)
        if kind == G2X:
            return remote(wout.at[u, c, qy, half_p], wout.at[u, c, qy, half_p], kind, slot, xn)
        if kind == G2Y:
            return remote(wout.at[u, c, qx, half_q], wout.at[u, c, qx, half_q], kind, slot, yn)
        q = {FX: qx, FY: qy, FD: qd}[kind]
        return remote(wout.at[u, c, q], wout.at[u, c, q], kind, slot, partner)

    def own_copies(u, slot):
        return (
            pltpu.make_async_copy(wnew.at[slot], wout.at[u, c, qm], out_sem.at[0, slot]),
            pltpu.make_async_copy(gbuf.at[slot], gout.at[u], out_sem.at[1, slot]),
        )

    def rows(i):
        return pl.ds(pl.multiple_of(i * B, B), B)

    def start_weights(jj, half):
        layer, j = 1 - jj // 3, jj % 3
        for i in range(4):
            ff = pl.ds(pl.multiple_of((4 * half + i) * 384 + j * 128, 128), 128)
            here = pl.ds(i * 128, 128)
            pltpu.make_async_copy(wg_hbm.at[layer, :, ff], wgv.at[half, :, here], weight_sem.at[half, 0]).start()
            pltpu.make_async_copy(wu_hbm.at[layer, :, ff], wuv.at[half, :, here], weight_sem.at[half, 1]).start()
            pltpu.make_async_copy(wd_hbm.at[layer, ff, :], wdv.at[half, here, :], weight_sem.at[half, 2]).start()

    def wait_weights(half):
        pltpu.make_async_copy(wgv.at[half], wgv.at[half], weight_sem.at[half, 0]).wait()
        pltpu.make_async_copy(wuv.at[half], wuv.at[half], weight_sem.at[half, 1]).wait()
        pltpu.make_async_copy(wdv.at[half], wdv.at[half], weight_sem.at[half, 2]).wait()

    def start_moments(jj, k):
        layer, j = 1 - jj // 3, jj % 3
        mine = pl.ds(pl.multiple_of(me * 96, 32), 96)
        for n, (bufs, refs) in enumerate(
            ((mbuf, (mg_hbm, mu_hbm, md_hbm)), (vbuf, (vg_hbm, vu_hbm, vd_hbm)), (wbuf, (wg_hbm, wu_hbm, wd_hbm)))
        ):
            sem = moment_sem.at[k, n]
            if k < 2:
                for mat in range(2):
                    for i in range(4):
                        ff = pl.ds(pl.multiple_of((4 * k + i) * 384 + j * 128, 128), 128)
                        src = refs[mat].at[layer, mine if n == 2 else slice(None), ff]
                        pltpu.make_async_copy(src, bufs.at[k, pl.ds(96 * mat, 96), pl.ds(128 * i, 128)], sem).start()
            else:
                first = j * 128 if n < 2 else me * 384 + j * 128
                for row, count, col, width, to_row, to_col in (
                    (0, 128, 0, 512, 0, 0),
                    (0, 64, 512, 256, 128, 0),
                    (64, 64, 512, 256, 128, 256),
                ):
                    src = refs[2].at[layer, pl.ds(pl.multiple_of(first + row, 64), count), pl.ds(col, width)]
                    pltpu.make_async_copy(src, bufs.at[k, pl.ds(to_row, count), pl.ds(to_col, width)], sem).start()

    def wait_moments(k):
        for n, bufs in enumerate((mbuf, vbuf, wbuf)):
            pltpu.make_async_copy(bufs.at[k], bufs.at[k], moment_sem.at[k, n]).wait()

    def f32(ref_value):
        return ref_value.astype(F32)

    def gather_stage(stage, jj, k):
        u, slot = 3 * jj + k, 3 * (jj % 2) + k
        top, low = slice(0, R // 2), slice(R // 2, R)
        if stage == 1:
            copy_of(S0, u, slot).wait_recv()
            grad[slot, c, qd] = (f32(grad[slot, c, qd]) + f32(recv0[slot, qd])).astype(BF)
        if stage == 2:
            start_moments(jj, k)
            copy_of(S1X, u, slot).wait_recv()
            copy_of(S1Y, u, slot).wait_recv()
            for q, with_p in ((qy, True), (qx, False)):
                for part, is_p in ((top, True), (low, False)):
                    total = f32(grad[slot, c, q, part]) + f32(recv0[slot, q, part])
                    if is_p and with_p:
                        total += f32(recv1[slot, 0])
                    if not is_p and not with_p:
                        total += f32(recv1[slot, 1])
                    grad[slot, c, q, part] = total.astype(BF)
        if stage == 3:
            wait_moments(k)
            copy_of(S2X, u, slot).wait_recv()
            copy_of(S2Y, u, slot).wait_recv()
            for part in (top, low):
                g = f32(grad[slot, c, qm, part]) + f32(recv0[slot, qm, part])
                g = (g + f32(recv2[slot, 0, part]) + f32(recv2[slot, 1, part])).astype(BF)
                gbuf[slot, part] = g
                g = g.astype(F32)
                m = 0.9 * mbuf[k, part] + 0.1 * g
                v = 0.95 * vbuf[k, part] + 0.05 * g * g
                w = f32(wbuf[k, part])
                wnew[slot, part] = (w - 0.02 * (m * lax.rsqrt(v + 1e-8) + 0.1 * w)).astype(BF)
            for kind in (S0, S1X, S1Y, S2X, S2Y):
                copy_of(kind, u, slot).wait_send()

    def send_stage(stage, jj, k):
        u, slot = 3 * jj + k, 3 * (jj % 2) + k
        if stage == 1:
            copy_of(S1X, u, slot).start()
            copy_of(S1Y, u, slot).start()
        if stage == 2:
            copy_of(S2X, u, slot).start()
            copy_of(S2Y, u, slot).start()
        if stage == 3:
            for kind in (G1X, G1Y, G1P):
                copy_of(kind, u, slot).start()
            for copy in own_copies(u, slot):
                copy.start()
        if stage == 4:
            copy_of(G1X, u, slot).wait_recv()
            copy_of(G1Y, u, slot).wait_recv()
            for kind in (G2X, G2Y, FX, FY):
                copy_of(kind, u, slot).start()
        if stage == 5:
            copy_of(G2X, u, slot).wait_recv()
            copy_of(G2Y, u, slot).wait_recv()
            copy_of(FD, u, slot).start()
        if stage == 6:
            for kind in (G1P, FX, FY, FD):
                copy_of(kind, u, slot).wait_recv()
            for kind in (G1X, G1Y, G1P, G2X, G2Y, FX, FY, FD):
                copy_of(kind, u, slot).wait_send()
            for copy in own_copies(u, slot):
                copy.wait()

    def tick(jj, p):
        active = []
        for stage in (3, 2, 1, 4, 5, 6):
            q, r = divmod(p - LAG * stage, 6)
            if r in (1, 4, 5):
                active.append((stage, jj + q, {1: 0, 4: 1, 5: 2}[r]))
        for stage, unit_jj, k in active:
            if stage <= 3:

                @pl.when((unit_jj >= 0) & (unit_jj < 6))
                def _():
                    gather_stage(stage, unit_jj, k)

        if p in (1, 4, 5):

            @pl.when(jj < 6)
            def _():
                k = {1: 0, 4: 1, 5: 2}[p]
                copy_of(S0, 3 * jj + k, 3 * (jj % 2) + k).start()

        for stage, unit_jj, k in active:

            @pl.when((unit_jj >= 0) & (unit_jj < 6))
            def _():
                send_stage(stage, unit_jj, k)

    def norm_states():
        @pl.loop(0, T // B)
        def _(i):
            wide = h[rows(i), :].astype(F32)
            value = (wide * scale_of(wide)).astype(BF)
            a[rows(i), :] = value
            at[:, rows(i)] = value.T

    def piece_hidden(half):
        wait_weights(half)

        @pl.loop(0, T // B)
        def _(i):
            here = a[rows(i), :]
            gate = nn(here, wgv[half])
            up = nn(here, wuv[half])
            dact = nt(ct[rows(i), :], wdv[half]).astype(BF).astype(F32)
            sig = jax.nn.sigmoid(gate)
            silu = gate * sig
            actt[:, rows(i)] = (silu * up).astype(BF).T
            dup[rows(i), :] = (dact * silu).astype(BF)
            dgate[rows(i), :] = (dact * up * (sig * (1.0 + gate * (1.0 - sig)))).astype(BF)

    def piece_gate_up(jj, half):
        slot = 3 * (jj % 2) + half
        for mat, z in enumerate((dgate, dup)):
            for n in range(2):
                term = nn(at[pl.ds(n * 384, 384), :], z[...]).astype(BF)
                for i in range(4):
                    d = 4 * n + i
                    grad[slot, d % 2, d // 2, pl.ds(96 * mat, 96), :] = term[96 * i : 96 * (i + 1)]

    def piece_down(jj, half):
        slot = 3 * (jj % 2) + 2
        for n in range(2):
            term = nn(actt[pl.ds(n * 256, 256), :], ct[...]).astype(BF)
            for i in range(2):
                d = 4 * half + 2 * n + i
                block = term[128 * i : 128 * (i + 1)]
                grad[slot, d % 2, d // 2, pl.ds(0, 128), :] = block[:, :512]
                grad[slot, d % 2, d // 2, pl.ds(128, 64), pl.ds(0, 256)] = block[:64, 512:]
                grad[slot, d % 2, d // 2, pl.ds(128, 64), pl.ds(256, 256)] = block[64:, 512:]

        @pl.when(jj < 3)
        def _():
            @pl.loop(0, T // B)
            def _(i):
                acc[rows(i), :] += nt(dgate[rows(i), :], wgv[half]) + nt(dup[rows(i), :], wuv[half])

    def next_layer():
        @pl.loop(0, T // B)
        def _(i):
            wide = h[rows(i), :].astype(F32)
            scale = scale_of(wide)
            da = acc[rows(i), :].astype(BF).astype(F32)
            dot = jnp.mean(da * wide, -1, keepdims=True)
            dh = (da * scale - wide * (scale * scale * scale * dot)).astype(BF)
            ct[rows(i), :] = ct[rows(i), :] + dh

        load = pltpu.make_async_copy(x_hbm, h, load_sem.at[0])
        load.start()
        load.wait()
        norm_states()

    loads = [pltpu.make_async_copy(h1_hbm, h, load_sem.at[0]), pltpu.make_async_copy(dy_hbm, ct, load_sem.at[1])]
    for load in loads:
        load.start()
    start_weights(0, 0)
    barrier = pltpu.get_barrier_semaphore()
    for device in (partner, xn, yn):
        pl.semaphore_signal(barrier, inc=1, device_id=(rep, device), device_id_type=pl.DeviceIdType.MESH)
    for load in loads:
        load.wait()
    norm_states()
    acc[...] = jnp.zeros_like(acc)
    pl.semaphore_wait(barrier, 3)

    @pl.loop(0, 8)
    def _(jj):
        @pl.when(jj == 3)
        def _():
            next_layer()

        for half in range(2):

            @pl.when(jj < 6)
            def _():
                if half == 0:
                    start_weights(jj, 1)
                else:

                    @pl.when(jj < 5)
                    def _():
                        start_weights(jj + 1, 0)

                piece_hidden(half)

            tick(jj, 3 * half)

            @pl.when(jj < 6)
            def _():
                piece_gate_up(jj, half)

            tick(jj, 3 * half + 1)

            @pl.when(jj < 6)
            def _():
                piece_down(jj, half)

            tick(jj, 3 * half + 2)


def train_step(x, h1, dy, *arrays):
    anywhere = pl.BlockSpec(memory_space=pl.ANY)
    block = (R, S)
    return pl.pallas_call(
        step_kernel,
        out_shape=(
            jax.ShapeDtypeStruct((UNITS, 2, 4) + block, BF),
            jax.ShapeDtypeStruct((UNITS,) + block, BF),
        ),
        in_specs=[anywhere] * 12,
        out_specs=(anywhere, anywhere),
        scratch_shapes=[
            pltpu.VMEM((T, D), BF),
            pltpu.VMEM((T, D), BF),
            pltpu.VMEM((D, T), BF),
            pltpu.VMEM((T, D), BF),
            pltpu.VMEM((T, D), F32),
            pltpu.VMEM((2, D, S), BF),
            pltpu.VMEM((2, D, S), BF),
            pltpu.VMEM((2, S, D), BF),
            pltpu.VMEM((S, T), BF),
            pltpu.VMEM((T, S), BF),
            pltpu.VMEM((T, S), BF),
            pltpu.VMEM((NS, 2, 4) + block, BF),
            pltpu.VMEM((NS, 4) + block, BF),
            pltpu.VMEM((NS, 2, R // 2, S), BF),
            pltpu.VMEM((NS, 2) + block, BF),
            pltpu.VMEM((3,) + block, F32),
            pltpu.VMEM((3,) + block, F32),
            pltpu.VMEM((3,) + block, BF),
            pltpu.VMEM((NS,) + block, BF),
            pltpu.VMEM((NS,) + block, BF),
            pltpu.SemaphoreType.DMA((KINDS, NS)),
            pltpu.SemaphoreType.DMA((KINDS, NS)),
            pltpu.SemaphoreType.DMA((2,)),
            pltpu.SemaphoreType.DMA((2, 3)),
            pltpu.SemaphoreType.DMA((3, 3)),
            pltpu.SemaphoreType.DMA((2, NS)),
        ],
        compiler_params=pltpu.CompilerParams(
            collective_id=0, has_side_effects=True, vmem_limit_bytes=VMEM_LIMIT
        ),
        name="train_step",
    )(x, h1, dy, *arrays)


def unpack_kernel(w_ref, g_ref, mg, mu, md, vg, vu, vd, gate, up, down, new_mg, new_mu, new_md, new_vg, new_vu, new_vd):
    d = pl.program_id(1)
    for j in range(3):
        for half in range(2):
            for i in range(4):
                to = pl.ds((4 * half + i) * 384 + j * 128, 128)
                gate[0, :, to] = w_ref[0, 3 * j + half, 0, 0, :96, i * 128 : (i + 1) * 128]
                up[0, :, to] = w_ref[0, 3 * j + half, 0, 0, 96:, i * 128 : (i + 1) * 128]
        down[0, pl.ds(j * 128, 128), :512] = w_ref[0, 3 * j + 2, 0, 0, :128, :]
        down[0, pl.ds(j * 128, 64), 512:] = w_ref[0, 3 * j + 2, 0, 0, 128:, :256]
        down[0, pl.ds(j * 128 + 64, 64), 512:] = w_ref[0, 3 * j + 2, 0, 0, 128:, 256:]

    def moments(g, m, v, new_m, new_v, at):
        g = g.astype(F32)
        new_m[at] = 0.9 * m[at] + 0.1 * g
        new_v[at] = 0.95 * v[at] + 0.05 * g * g

    lanes = pl.ds(pl.multiple_of((d % 4) * 128, 128), 128)
    for j in range(3):
        at = (0, slice(None), slice(j * 128, (j + 1) * 128))
        moments(g_ref[0, 3 * j + d // 4, :96, lanes], mg, vg, new_mg, new_vg, at)
        moments(g_ref[0, 3 * j + d // 4, 96:, lanes], mu, vu, new_mu, new_vu, at)

    @pl.when(d < 3)
    def _():
        for row, count, col, width, to_row, to_col in ((0, 128, 0, 512, 0, 0), (128, 64, 0, 256, 0, 512), (128, 64, 256, 256, 64, 512)):
            g = g_ref[0, 3 * d + 2, row : row + count, col : col + width]
            moments(g, md, vd, new_md, new_vd, (0, slice(to_row, to_row + count), slice(to_col, to_col + width)))


def unpack(wout, gout, mg, mu, md, vg, vu, vd):
    w_spec = pl.BlockSpec((1, 9, 1, 1, R, S), lambda l, d: (1 - l, 0, d % 2, d // 2, 0, 0))
    g_spec = pl.BlockSpec((1, 9, R, S), lambda l, d: (1 - l, 0, 0, 0))
    wide = pl.BlockSpec((1, 96, FF), lambda l, d: (l, d, 0))
    tall = pl.BlockSpec((1, 384, D), lambda l, d: (l, d, 0))
    m_wide = pl.BlockSpec((1, 96, 384), lambda l, d: (l, 0, d))
    m_tall = pl.BlockSpec((1, 128, D), lambda l, d: (l, jnp.minimum(d, 2), 0))
    m_specs = [m_wide, m_wide, m_tall] * 2
    moments = (mg, mu, md, vg, vu, vd)
    return pl.pallas_call(
        unpack_kernel,
        grid=(2, 8),
        out_shape=[jax.ShapeDtypeStruct(s, BF) for s in ((2, D, FF), (2, D, FF), (2, FF, D))]
        + [jax.ShapeDtypeStruct(m.shape, F32) for m in moments],
        in_specs=[w_spec, g_spec] + m_specs,
        out_specs=[wide, wide, tall] + m_specs,
        compiler_params=pltpu.CompilerParams(vmem_limit_bytes=56_000_000),
        name="unpack",
    )(wout.reshape(2, 9, 2, 4, R, S), gout.reshape(2, 9, R, S), *moments)


def solution(mesh):
    def body(x, dy, wg, wu, wd, mg, mu, md, vg, vu, vd):
        h1 = forward(x[0], wg, wu, wd)
        wout, gout = train_step(x[0], h1, dy[0], wg, wu, wd, mg, mu, md, vg, vu, vd)
        return tuple(unpack(wout, gout, mg, mu, md, vg, vu, vd))

    tok, whole, rows = P(("rep", "dp")), P(), P(None, "dp")
    return jax.shard_map(
        body,
        mesh=mesh,
        in_specs=(tok, tok) + (whole,) * 3 + (rows,) * 6,
        out_specs=(P("rep"),) * 3 + (P("rep", "dp"),) * 6,
        check_vma=False,
    )
```

```python
import jax
import jax.numpy as jnp
from jax import lax
from jax.experimental import pallas as pl
from jax.experimental.pallas import tpu as pltpu
from jax.sharding import PartitionSpec as P

T, D, FF = 2048, 768, 3072
S = 512
B = 512
R = 192
NS = 6
LAGS = (0, 1, 2, 4, 6, 8, 10)
UNITS = 18
VMEM_LIMIT = 66_500_000
BF, F32 = jnp.bfloat16, jnp.float32


def nn(a, b):
    return jnp.dot(a, b, preferred_element_type=F32)


def nt(a, b):
    return lax.dot_general(a, b, (((1,), (1,)), ((), ())), preferred_element_type=F32)


def scale_of(wide):
    return lax.rsqrt(jnp.mean(wide * wide, -1, keepdims=True) + 1e-6)


S0, S1X, S1Y, S2X, S2Y, G1X, G1Y, G1P, G2X, G2Y, FX, FY, FD = range(13)
KINDS = 13


def step_kernel(
    x_hbm, dy_hbm, wg_hbm, wu_hbm, wd_hbm, mg_hbm, mu_hbm, md_hbm, vg_hbm, vu_hbm, vd_hbm,
    wout, gout,
    h, a, at, ct, acc, wgv, wuv, wdv, actt, dgate, dup,
    grad, recv0, recv1, recv2, mbuf, vbuf, wbuf, wnew, gbuf,
    send_sem, recv_sem, load_sem, weight_sem, moment_sem, out_sem,
):
    rep, me = lax.axis_index("rep"), lax.axis_index("dp")
    c, qm = me % 2, me // 2
    qx, qy = (qm + 2) % 4, qm + 1 - 2 * (qm % 2)
    qd = (qy + 2) % 4
    partner, xn, yn = 2 * qm + 1 - c, 2 * qx + c, 2 * qy + c

    def remote(src, dst, kind, slot, device):
        return pltpu.make_async_remote_copy(
            src_ref=src, dst_ref=dst, send_sem=send_sem.at[kind, slot], recv_sem=recv_sem.at[kind, slot],
            device_id=(rep, device), device_id_type=pl.DeviceIdType.MESH,
        )

    half_p, half_q = pl.ds(0, R // 2), pl.ds(R // 2, R // 2)

    def copy_of(kind, u, slot):
        if kind == S0:
            return remote(grad.at[slot, 1 - c], recv0.at[slot], kind, slot, partner)
        if kind == S1X:
            return remote(grad.at[slot, c, qd, half_p], recv1.at[slot, 0], kind, slot, xn)
        if kind == S1Y:
            return remote(grad.at[slot, c, qd, half_q], recv1.at[slot, 1], kind, slot, yn)
        if kind == S2X:
            return remote(grad.at[slot, c, qx], recv2.at[slot, 0], kind, slot, xn)
        if kind == S2Y:
            return remote(grad.at[slot, c, qy], recv2.at[slot, 1], kind, slot, yn)
        if kind in (G1X, G1Y, G1P):
            to = {G1X: xn, G1Y: yn, G1P: partner}[kind]
            return remote(wnew.at[slot], wout.at[u, c, qm], kind, slot, to)
        if kind == G2X:
            return remote(wout.at[u, c, qy, half_p], wout.at[u, c, qy, half_p], kind, slot, xn)
        if kind == G2Y:
            return remote(wout.at[u, c, qx, half_q], wout.at[u, c, qx, half_q], kind, slot, yn)
        q = {FX: qx, FY: qy, FD: qd}[kind]
        return remote(wout.at[u, c, q], wout.at[u, c, q], kind, slot, partner)

    def own_copies(u, slot):
        return (
            pltpu.make_async_copy(wnew.at[slot], wout.at[u, c, qm], out_sem.at[0, slot]),
            pltpu.make_async_copy(gbuf.at[slot], gout.at[u], out_sem.at[1, slot]),
        )

    def rows(i):
        return pl.ds(pl.multiple_of(i * B, B), B)

    def start_weights(jj, half):
        layer, j = 1 - jj // 3, jj % 3
        for i in range(4):
            ff = pl.ds(pl.multiple_of((4 * half + i) * 384 + j * 128, 128), 128)
            here = pl.ds(i * 128, 128)
            pltpu.make_async_copy(wg_hbm.at[layer, :, ff], wgv.at[half, :, here], weight_sem.at[half, 0]).start()
            pltpu.make_async_copy(wu_hbm.at[layer, :, ff], wuv.at[half, :, here], weight_sem.at[half, 1]).start()
            pltpu.make_async_copy(wd_hbm.at[layer, ff, :], wdv.at[half, here, :], weight_sem.at[half, 2]).start()

    def wait_weights(half):
        pltpu.make_async_copy(wgv.at[half], wgv.at[half], weight_sem.at[half, 0]).wait()
        pltpu.make_async_copy(wuv.at[half], wuv.at[half], weight_sem.at[half, 1]).wait()
        pltpu.make_async_copy(wdv.at[half], wdv.at[half], weight_sem.at[half, 2]).wait()

    def start_moments(jj, k):
        layer, j = 1 - jj // 3, jj % 3
        mine = pl.ds(pl.multiple_of(me * 96, 32), 96)
        for n, (bufs, refs) in enumerate(
            ((mbuf, (mg_hbm, mu_hbm, md_hbm)), (vbuf, (vg_hbm, vu_hbm, vd_hbm)), (wbuf, (wg_hbm, wu_hbm, wd_hbm)))
        ):
            sem = moment_sem.at[k, n]
            if k < 2:
                for mat in range(2):
                    for i in range(4):
                        ff = pl.ds(pl.multiple_of((4 * k + i) * 384 + j * 128, 128), 128)
                        src = refs[mat].at[layer, mine if n == 2 else slice(None), ff]
                        pltpu.make_async_copy(src, bufs.at[k, pl.ds(96 * mat, 96), pl.ds(128 * i, 128)], sem).start()
            else:
                first = j * 128 if n < 2 else me * 384 + j * 128
                for row, count, col, width, to_row, to_col in (
                    (0, 128, 0, 512, 0, 0),
                    (0, 64, 512, 256, 128, 0),
                    (64, 64, 512, 256, 128, 256),
                ):
                    src = refs[2].at[layer, pl.ds(pl.multiple_of(first + row, 64), count), pl.ds(col, width)]
                    pltpu.make_async_copy(src, bufs.at[k, pl.ds(to_row, count), pl.ds(to_col, width)], sem).start()

    def wait_moments(k):
        for n, bufs in enumerate((mbuf, vbuf, wbuf)):
            pltpu.make_async_copy(bufs.at[k], bufs.at[k], moment_sem.at[k, n]).wait()

    def f32(ref_value):
        return ref_value.astype(F32)

    def gather_stage(stage, jj, k):
        u, slot = 3 * jj + k, 3 * (jj % 2) + k
        top, low = slice(0, R // 2), slice(R // 2, R)
        if stage == 1:
            copy_of(S0, u, slot).wait_recv()
            grad[slot, c, qd] = (f32(grad[slot, c, qd]) + f32(recv0[slot, qd])).astype(BF)
        if stage == 2:
            start_moments(jj, k)
            copy_of(S1X, u, slot).wait_recv()
            copy_of(S1Y, u, slot).wait_recv()
            for q, with_p in ((qy, True), (qx, False)):
                for part, is_p in ((top, True), (low, False)):
                    total = f32(grad[slot, c, q, part]) + f32(recv0[slot, q, part])
                    if is_p and with_p:
                        total += f32(recv1[slot, 0])
                    if not is_p and not with_p:
                        total += f32(recv1[slot, 1])
                    grad[slot, c, q, part] = total.astype(BF)
        if stage == 3:
            wait_moments(k)
            copy_of(S2X, u, slot).wait_recv()
            copy_of(S2Y, u, slot).wait_recv()
            for part in (top, low):
                g = f32(grad[slot, c, qm, part]) + f32(recv0[slot, qm, part])
                g = (g + f32(recv2[slot, 0, part]) + f32(recv2[slot, 1, part])).astype(BF)
                gbuf[slot, part] = g
                g = g.astype(F32)
                m = 0.9 * mbuf[k, part] + 0.1 * g
                v = 0.95 * vbuf[k, part] + 0.05 * g * g
                w = f32(wbuf[k, part])
                wnew[slot, part] = (w - 0.02 * (m * lax.rsqrt(v + 1e-8) + 0.1 * w)).astype(BF)
            for kind in (S0, S1X, S1Y, S2X, S2Y):
                copy_of(kind, u, slot).wait_send()

    def send_stage(stage, jj, k):
        u, slot = 3 * jj + k, 3 * (jj % 2) + k
        if stage == 1:
            copy_of(S1X, u, slot).start()
            copy_of(S1Y, u, slot).start()
        if stage == 2:
            copy_of(S2X, u, slot).start()
            copy_of(S2Y, u, slot).start()
        if stage == 3:
            for kind in (G1X, G1Y, G1P):
                copy_of(kind, u, slot).start()
            for copy in own_copies(u, slot):
                copy.start()
        if stage == 4:
            copy_of(G1X, u, slot).wait_recv()
            copy_of(G1Y, u, slot).wait_recv()
            for kind in (G2X, G2Y, FX, FY):
                copy_of(kind, u, slot).start()
        if stage == 5:
            copy_of(G2X, u, slot).wait_recv()
            copy_of(G2Y, u, slot).wait_recv()
            copy_of(FD, u, slot).start()
        if stage == 6:
            for kind in (G1P, FX, FY, FD):
                copy_of(kind, u, slot).wait_recv()
            for kind in (G1X, G1Y, G1P, G2X, G2Y, FX, FY, FD):
                copy_of(kind, u, slot).wait_send()
            for copy in own_copies(u, slot):
                copy.wait()

    def tick(jj, p):
        active = []
        for stage in range(1, 7):
            q, r = divmod(p - LAGS[stage], 6)
            if r in (1, 4, 5):
                active.append((stage, jj + q, {1: 0, 4: 1, 5: 2}[r]))
        for stage, unit_jj, k in active:
            if stage <= 3:

                @pl.when((unit_jj >= 0) & (unit_jj < 6))
                def _():
                    gather_stage(stage, unit_jj, k)

        if p in (1, 4, 5):

            @pl.when(jj < 6)
            def _():
                k = {1: 0, 4: 1, 5: 2}[p]
                copy_of(S0, 3 * jj + k, 3 * (jj % 2) + k).start()

        for stage, unit_jj, k in active:

            @pl.when((unit_jj >= 0) & (unit_jj < 6))
            def _():
                send_stage(stage, unit_jj, k)

    def norm_states():
        @pl.loop(0, T // B)
        def _(i):
            wide = h[rows(i), :].astype(F32)
            value = (wide * scale_of(wide)).astype(BF)
            a[rows(i), :] = value
            at[:, rows(i)] = value.T

    def piece_hidden(half):
        wait_weights(half)

        @pl.loop(0, T // B)
        def _(i):
            here = a[rows(i), :]
            gate = nn(here, wgv[half])
            up = nn(here, wuv[half])
            dact = nt(ct[rows(i), :], wdv[half]).astype(BF).astype(F32)
            sig = jax.nn.sigmoid(gate)
            silu = gate * sig
            actt[:, rows(i)] = (silu * up).astype(BF).T
            dup[rows(i), :] = (dact * silu).astype(BF)
            dgate[rows(i), :] = (dact * up * (sig * (1.0 + gate * (1.0 - sig)))).astype(BF)

    def piece_gate_up(jj, half):
        slot = 3 * (jj % 2) + half
        for mat, z in enumerate((dgate, dup)):
            for n in range(2):
                term = nn(at[pl.ds(n * 384, 384), :], z[...]).astype(BF)
                for i in range(4):
                    d = 4 * n + i
                    grad[slot, d % 2, d // 2, pl.ds(96 * mat, 96), :] = term[96 * i : 96 * (i + 1)]

    def piece_down(jj, half):
        slot = 3 * (jj % 2) + 2
        for n in range(2):
            term = nn(actt[pl.ds(n * 256, 256), :], ct[...]).astype(BF)
            for i in range(2):
                d = 4 * half + 2 * n + i
                block = term[128 * i : 128 * (i + 1)]
                grad[slot, d % 2, d // 2, pl.ds(0, 128), :] = block[:, :512]
                grad[slot, d % 2, d // 2, pl.ds(128, 64), pl.ds(0, 256)] = block[:64, 512:]
                grad[slot, d % 2, d // 2, pl.ds(128, 64), pl.ds(256, 256)] = block[64:, 512:]

        @pl.when(jj < 3)
        def _():
            @pl.loop(0, T // B)
            def _(i):
                acc[rows(i), :] += nt(dgate[rows(i), :], wgv[half]) + nt(dup[rows(i), :], wuv[half])

    def next_layer():
        @pl.loop(0, T // B)
        def _(i):
            wide = h[rows(i), :].astype(F32)
            scale = scale_of(wide)
            da = acc[rows(i), :].astype(BF).astype(F32)
            dot = jnp.mean(da * wide, -1, keepdims=True)
            dh = (da * scale - wide * (scale * scale * scale * dot)).astype(BF)
            ct[rows(i), :] = ct[rows(i), :] + dh

        load = pltpu.make_async_copy(x_hbm, h, load_sem.at[0])
        load.start()
        load.wait()
        norm_states()

    def start_forward(block, half):
        ff = pl.ds(pl.multiple_of(block * S, S), S)
        pltpu.make_async_copy(wg_hbm.at[0, :, ff], wgv.at[half], weight_sem.at[half, 0]).start()
        pltpu.make_async_copy(wu_hbm.at[0, :, ff], wuv.at[half], weight_sem.at[half, 1]).start()
        pltpu.make_async_copy(wd_hbm.at[0, ff, :], wdv.at[half], weight_sem.at[half, 2]).start()

    def piece_forward(half):
        wait_weights(half)

        @pl.loop(0, T // B)
        def _(i):
            here = a[rows(i), :]
            gate = nn(here, wgv[half])
            up = nn(here, wuv[half])
            act = (gate * jax.nn.sigmoid(gate) * up).astype(BF)
            acc[rows(i), :] += nn(act, wdv[half])

    loads = [pltpu.make_async_copy(x_hbm, h, load_sem.at[0]), pltpu.make_async_copy(dy_hbm, ct, load_sem.at[1])]
    loads[0].start()
    start_forward(0, 0)
    loads[1].start()
    barrier = pltpu.get_barrier_semaphore()
    for device in (partner, xn, yn):
        pl.semaphore_signal(barrier, inc=1, device_id=(rep, device), device_id_type=pl.DeviceIdType.MESH)
    loads[0].wait()

    @pl.loop(0, T // B)
    def _(i):
        wide = h[rows(i), :].astype(F32)
        a[rows(i), :] = (wide * scale_of(wide)).astype(BF)
        acc[rows(i), :] = jnp.zeros((B, D), F32)

    @pl.loop(0, FF // S // 2)
    def _(pair):
        start_forward(2 * pair + 1, 1)
        piece_forward(0)

        @pl.when(pair < FF // S // 2 - 1)
        def _():
            start_forward(2 * pair + 2, 0)

        @pl.when(pair == FF // S // 2 - 1)
        def _():
            start_weights(0, 0)

        piece_forward(1)

    @pl.loop(0, T // B)
    def _(i):
        h[rows(i), :] = h[rows(i), :] + acc[rows(i), :].astype(BF)
        acc[rows(i), :] = jnp.zeros((B, D), F32)

    norm_states()
    loads[1].wait()
    pl.semaphore_wait(barrier, 3)

    @pl.loop(0, 8)
    def _(jj):
        @pl.when(jj == 3)
        def _():
            next_layer()

        for half in range(2):

            @pl.when(jj < 6)
            def _():
                if half == 0:
                    start_weights(jj, 1)
                else:

                    @pl.when(jj < 5)
                    def _():
                        start_weights(jj + 1, 0)

                piece_hidden(half)

            tick(jj, 3 * half)

            @pl.when(jj < 6)
            def _():
                piece_gate_up(jj, half)

            tick(jj, 3 * half + 1)

            @pl.when(jj < 6)
            def _():
                piece_down(jj, half)

            tick(jj, 3 * half + 2)


def train_step(x, dy, *arrays):
    anywhere = pl.BlockSpec(memory_space=pl.ANY)
    block = (R, S)
    return pl.pallas_call(
        step_kernel,
        out_shape=(
            jax.ShapeDtypeStruct((UNITS, 2, 4) + block, BF),
            jax.ShapeDtypeStruct((UNITS,) + block, BF),
        ),
        in_specs=[anywhere] * 11,
        out_specs=(anywhere, anywhere),
        scratch_shapes=[
            pltpu.VMEM((T, D), BF),
            pltpu.VMEM((T, D), BF),
            pltpu.VMEM((D, T), BF),
            pltpu.VMEM((T, D), BF),
            pltpu.VMEM((T, D), F32),
            pltpu.VMEM((2, D, S), BF),
            pltpu.VMEM((2, D, S), BF),
            pltpu.VMEM((2, S, D), BF),
            pltpu.VMEM((S, T), BF),
            pltpu.VMEM((T, S), BF),
            pltpu.VMEM((T, S), BF),
            pltpu.VMEM((NS, 2, 4) + block, BF),
            pltpu.VMEM((NS, 4) + block, BF),
            pltpu.VMEM((NS, 2, R // 2, S), BF),
            pltpu.VMEM((NS, 2) + block, BF),
            pltpu.VMEM((3,) + block, F32),
            pltpu.VMEM((3,) + block, F32),
            pltpu.VMEM((3,) + block, BF),
            pltpu.VMEM((NS,) + block, BF),
            pltpu.VMEM((NS,) + block, BF),
            pltpu.SemaphoreType.DMA((KINDS, NS)),
            pltpu.SemaphoreType.DMA((KINDS, NS)),
            pltpu.SemaphoreType.DMA((2,)),
            pltpu.SemaphoreType.DMA((2, 3)),
            pltpu.SemaphoreType.DMA((3, 3)),
            pltpu.SemaphoreType.DMA((2, NS)),
        ],
        compiler_params=pltpu.CompilerParams(
            collective_id=0, has_side_effects=True, vmem_limit_bytes=VMEM_LIMIT
        ),
        name="train_step",
    )(x, dy, *arrays)


def unpack_kernel(w_ref, g_ref, mg, mu, md, vg, vu, vd, gate, up, down, new_mg, new_mu, new_md, new_vg, new_vu, new_vd):
    d = pl.program_id(1)
    for j in range(3):
        for half in range(2):
            for i in range(4):
                to = pl.ds((4 * half + i) * 384 + j * 128, 128)
                gate[0, :, to] = w_ref[0, 3 * j + half, 0, 0, :96, i * 128 : (i + 1) * 128]
                up[0, :, to] = w_ref[0, 3 * j + half, 0, 0, 96:, i * 128 : (i + 1) * 128]
        down[0, pl.ds(j * 128, 128), :512] = w_ref[0, 3 * j + 2, 0, 0, :128, :]
        down[0, pl.ds(j * 128, 64), 512:] = w_ref[0, 3 * j + 2, 0, 0, 128:, :256]
        down[0, pl.ds(j * 128 + 64, 64), 512:] = w_ref[0, 3 * j + 2, 0, 0, 128:, 256:]

    def moments(g, m, v, new_m, new_v, at):
        g = g.astype(F32)
        new_m[at] = 0.9 * m[at] + 0.1 * g
        new_v[at] = 0.95 * v[at] + 0.05 * g * g

    lanes = pl.ds(pl.multiple_of((d % 4) * 128, 128), 128)
    for j in range(3):
        at = (0, slice(None), slice(j * 128, (j + 1) * 128))
        moments(g_ref[0, 3 * j + d // 4, :96, lanes], mg, vg, new_mg, new_vg, at)
        moments(g_ref[0, 3 * j + d // 4, 96:, lanes], mu, vu, new_mu, new_vu, at)

    @pl.when(d < 3)
    def _():
        for row, count, col, width, to_row, to_col in ((0, 128, 0, 512, 0, 0), (128, 64, 0, 256, 0, 512), (128, 64, 256, 256, 64, 512)):
            g = g_ref[0, 3 * d + 2, row : row + count, col : col + width]
            moments(g, md, vd, new_md, new_vd, (0, slice(to_row, to_row + count), slice(to_col, to_col + width)))


def unpack(wout, gout, mg, mu, md, vg, vu, vd):
    w_spec = pl.BlockSpec((1, 9, 1, 1, R, S), lambda l, d: (1 - l, 0, d % 2, d // 2, 0, 0))
    g_spec = pl.BlockSpec((1, 9, R, S), lambda l, d: (1 - l, 0, 0, 0))
    wide = pl.BlockSpec((1, 96, FF), lambda l, d: (l, d, 0))
    tall = pl.BlockSpec((1, 384, D), lambda l, d: (l, d, 0))
    m_wide = pl.BlockSpec((1, 96, 384), lambda l, d: (l, 0, d))
    m_tall = pl.BlockSpec((1, 128, D), lambda l, d: (l, jnp.minimum(d, 2), 0))
    m_specs = [m_wide, m_wide, m_tall] * 2
    moments = (mg, mu, md, vg, vu, vd)
    return pl.pallas_call(
        unpack_kernel,
        grid=(2, 8),
        out_shape=[jax.ShapeDtypeStruct(s, BF) for s in ((2, D, FF), (2, D, FF), (2, FF, D))]
        + [jax.ShapeDtypeStruct(m.shape, F32) for m in moments],
        in_specs=[w_spec, g_spec] + m_specs,
        out_specs=[wide, wide, tall] + m_specs,
        compiler_params=pltpu.CompilerParams(vmem_limit_bytes=56_000_000),
        name="unpack",
    )(wout.reshape(2, 9, 2, 4, R, S), gout.reshape(2, 9, R, S), *moments)


def solution(mesh):
    def body(x, dy, wg, wu, wd, mg, mu, md, vg, vu, vd):
        wout, gout = train_step(x[0], dy[0], wg, wu, wd, mg, mu, md, vg, vu, vd)
        return tuple(unpack(wout, gout, mg, mu, md, vg, vu, vd))

    tok, whole, rows = P(("rep", "dp")), P(), P(None, "dp")
    return jax.shard_map(
        body,
        mesh=mesh,
        in_specs=(tok, tok) + (whole,) * 3 + (rows,) * 6,
        out_specs=(P("rep"),) * 3 + (P("rep", "dp"),) * 6,
        check_vma=False,
    )
```

```python
import jax
import jax.numpy as jnp
from jax import lax
from jax.experimental import pallas as pl
from jax.experimental.pallas import tpu as pltpu
from jax.sharding import PartitionSpec as P

T, D, FF = 2048, 768, 3072
S = 512
B = 512
R = 192
NS = 6
LAGS = (0, 1, 2, 4, 6, 8, 10)
UNITS = 18
VMEM_LIMIT = 66_500_000
BF, F32 = jnp.bfloat16, jnp.float32


def nn(a, b):
    return jnp.dot(a, b, preferred_element_type=F32)


def nt(a, b):
    return lax.dot_general(a, b, (((1,), (1,)), ((), ())), preferred_element_type=F32)


def scale_of(wide):
    return lax.rsqrt(jnp.mean(wide * wide, -1, keepdims=True) + 1e-6)


S0, S1X, S1Y, S2X, S2Y, G1X, G1Y, G1P, G2X, G2Y, FX, FY, FD = range(13)
KINDS = 13


def step_kernel(
    x_hbm, dy_hbm, wg_hbm, wu_hbm, wd_hbm, mg_hbm, mu_hbm, md_hbm, vg_hbm, vu_hbm, vd_hbm,
    wout, gout,
    h, a, at, ct, acc, wgv, wuv, wdv, actt, dgate, dup,
    grad, recv0, recv1, recv2, mbuf, vbuf, wbuf, wnew, gbuf,
    send_sem, recv_sem, load_sem, weight_sem, moment_sem, out_sem,
):
    rep, me = lax.axis_index("rep"), lax.axis_index("dp")
    c, qm = me % 2, me // 2
    qx, qy = (qm + 2) % 4, qm + 1 - 2 * (qm % 2)
    qd = (qy + 2) % 4
    partner, xn, yn = 2 * qm + 1 - c, 2 * qx + c, 2 * qy + c

    def remote(src, dst, kind, slot, device):
        return pltpu.make_async_remote_copy(
            src_ref=src, dst_ref=dst, send_sem=send_sem.at[kind, slot], recv_sem=recv_sem.at[kind, slot],
            device_id=(rep, device), device_id_type=pl.DeviceIdType.MESH,
        )

    half_p, half_q = pl.ds(0, R // 2), pl.ds(R // 2, R // 2)

    def copy_of(kind, u, slot):
        if kind == S0:
            return remote(grad.at[slot, 1 - c], recv0.at[slot], kind, slot, partner)
        if kind == S1X:
            return remote(grad.at[slot, c, qd, half_p], recv1.at[slot, 0], kind, slot, xn)
        if kind == S1Y:
            return remote(grad.at[slot, c, qd, half_q], recv1.at[slot, 1], kind, slot, yn)
        if kind == S2X:
            return remote(grad.at[slot, c, qx], recv2.at[slot, 0], kind, slot, xn)
        if kind == S2Y:
            return remote(grad.at[slot, c, qy], recv2.at[slot, 1], kind, slot, yn)
        if kind in (G1X, G1Y, G1P):
            to = {G1X: xn, G1Y: yn, G1P: partner}[kind]
            return remote(wnew.at[slot], wout.at[u, c, qm], kind, slot, to)
        if kind == G2X:
            return remote(wout.at[u, c, qy, half_p], wout.at[u, c, qy, half_p], kind, slot, xn)
        if kind == G2Y:
            return remote(wout.at[u, c, qx, half_q], wout.at[u, c, qx, half_q], kind, slot, yn)
        q = {FX: qx, FY: qy, FD: qd}[kind]
        return remote(wout.at[u, c, q], wout.at[u, c, q], kind, slot, partner)

    def own_copies(u, slot):
        return (
            pltpu.make_async_copy(wnew.at[slot], wout.at[u, c, qm], out_sem.at[0, slot]),
            pltpu.make_async_copy(gbuf.at[slot], gout.at[u], out_sem.at[1, slot]),
        )

    def rows(i):
        return pl.ds(pl.multiple_of(i * B, B), B)

    def start_weights(jj, half):
        layer, j = 1 - jj // 3, jj % 3
        for i in range(4):
            ff = pl.ds(pl.multiple_of((4 * half + i) * 384 + j * 128, 128), 128)
            here = pl.ds(i * 128, 128)
            pltpu.make_async_copy(wg_hbm.at[layer, :, ff], wgv.at[half, :, here], weight_sem.at[half, 0]).start()
            pltpu.make_async_copy(wu_hbm.at[layer, :, ff], wuv.at[half, :, here], weight_sem.at[half, 1]).start()
            pltpu.make_async_copy(wd_hbm.at[layer, ff, :], wdv.at[half, here, :], weight_sem.at[half, 2]).start()

    def wait_weights(half):
        pltpu.make_async_copy(wgv.at[half], wgv.at[half], weight_sem.at[half, 0]).wait()
        pltpu.make_async_copy(wuv.at[half], wuv.at[half], weight_sem.at[half, 1]).wait()
        pltpu.make_async_copy(wdv.at[half], wdv.at[half], weight_sem.at[half, 2]).wait()

    def start_moments(jj, k):
        layer, j = 1 - jj // 3, jj % 3
        mine = pl.ds(pl.multiple_of(me * 96, 32), 96)
        for n, (bufs, refs) in enumerate(
            ((mbuf, (mg_hbm, mu_hbm, md_hbm)), (vbuf, (vg_hbm, vu_hbm, vd_hbm)), (wbuf, (wg_hbm, wu_hbm, wd_hbm)))
        ):
            sem = moment_sem.at[k, n]
            if k < 2:
                for mat in range(2):
                    for i in range(4):
                        ff = pl.ds(pl.multiple_of((4 * k + i) * 384 + j * 128, 128), 128)
                        src = refs[mat].at[layer, mine if n == 2 else slice(None), ff]
                        pltpu.make_async_copy(src, bufs.at[k, pl.ds(96 * mat, 96), pl.ds(128 * i, 128)], sem).start()
            else:
                first = j * 128 if n < 2 else me * 384 + j * 128
                for row, count, col, width, to_row, to_col in (
                    (0, 128, 0, 512, 0, 0),
                    (0, 64, 512, 256, 128, 0),
                    (64, 64, 512, 256, 128, 256),
                ):
                    src = refs[2].at[layer, pl.ds(pl.multiple_of(first + row, 64), count), pl.ds(col, width)]
                    pltpu.make_async_copy(src, bufs.at[k, pl.ds(to_row, count), pl.ds(to_col, width)], sem).start()

    def wait_moments(k):
        for n, bufs in enumerate((mbuf, vbuf, wbuf)):
            pltpu.make_async_copy(bufs.at[k], bufs.at[k], moment_sem.at[k, n]).wait()

    def f32(ref_value):
        return ref_value.astype(F32)

    def gather_stage(stage, jj, k):
        u, slot = 3 * jj + k, 3 * (jj % 2) + k
        top, low = slice(0, R // 2), slice(R // 2, R)
        if stage == 1:
            copy_of(S0, u, slot).wait_recv()
            grad[slot, c, qd] = (f32(grad[slot, c, qd]) + f32(recv0[slot, qd])).astype(BF)
        if stage == 2:
            start_moments(jj, k)
            copy_of(S1X, u, slot).wait_recv()
            copy_of(S1Y, u, slot).wait_recv()
            for q, with_p in ((qy, True), (qx, False)):
                for part, is_p in ((top, True), (low, False)):
                    total = f32(grad[slot, c, q, part]) + f32(recv0[slot, q, part])
                    if is_p and with_p:
                        total += f32(recv1[slot, 0])
                    if not is_p and not with_p:
                        total += f32(recv1[slot, 1])
                    grad[slot, c, q, part] = total.astype(BF)
        if stage == 3:
            wait_moments(k)
            copy_of(S2X, u, slot).wait_recv()
            copy_of(S2Y, u, slot).wait_recv()
            for part in (top, low):
                g = f32(grad[slot, c, qm, part]) + f32(recv0[slot, qm, part])
                g = (g + f32(recv2[slot, 0, part]) + f32(recv2[slot, 1, part])).astype(BF)
                gbuf[slot, part] = g
                g = g.astype(F32)
                m = 0.9 * mbuf[k, part] + 0.1 * g
                v = 0.95 * vbuf[k, part] + 0.05 * g * g
                w = f32(wbuf[k, part])
                wnew[slot, part] = (w - 0.02 * (m * lax.rsqrt(v + 1e-8) + 0.1 * w)).astype(BF)
            for kind in (S0, S1X, S1Y, S2X, S2Y):
                copy_of(kind, u, slot).wait_send()

    def send_stage(stage, jj, k):
        u, slot = 3 * jj + k, 3 * (jj % 2) + k
        if stage == 1:
            copy_of(S1X, u, slot).start()
            copy_of(S1Y, u, slot).start()
        if stage == 2:
            copy_of(S2X, u, slot).start()
            copy_of(S2Y, u, slot).start()
        if stage == 3:
            for kind in (G1X, G1Y, G1P):
                copy_of(kind, u, slot).start()
            for copy in own_copies(u, slot):
                copy.start()
        if stage == 4:
            copy_of(G1X, u, slot).wait_recv()
            copy_of(G1Y, u, slot).wait_recv()
            for kind in (G2X, G2Y, FX, FY):
                copy_of(kind, u, slot).start()
        if stage == 5:
            copy_of(G2X, u, slot).wait_recv()
            copy_of(G2Y, u, slot).wait_recv()
            copy_of(FD, u, slot).start()
        if stage == 6:
            for kind in (G1P, FX, FY, FD):
                copy_of(kind, u, slot).wait_recv()
            for kind in (G1X, G1Y, G1P, G2X, G2Y, FX, FY, FD):
                copy_of(kind, u, slot).wait_send()
            for copy in own_copies(u, slot):
                copy.wait()

    def tick(jj, p):
        active = []
        for stage in range(1, 7):
            q, r = divmod(p - LAGS[stage], 6)
            if r in (1, 4, 5):
                active.append((stage, jj + q, {1: 0, 4: 1, 5: 2}[r]))
        for stage, unit_jj, k in active:
            if stage <= 3:

                @pl.when((unit_jj >= 0) & (unit_jj < 6))
                def _():
                    gather_stage(stage, unit_jj, k)

        if p in (1, 4, 5):

            @pl.when(jj < 6)
            def _():
                k = {1: 0, 4: 1, 5: 2}[p]
                copy_of(S0, 3 * jj + k, 3 * (jj % 2) + k).start()

        for stage, unit_jj, k in active:

            @pl.when((unit_jj >= 0) & (unit_jj < 6))
            def _():
                send_stage(stage, unit_jj, k)

    def norm_states():
        @pl.loop(0, T // B)
        def _(i):
            wide = h[rows(i), :].astype(F32)
            value = (wide * scale_of(wide)).astype(BF)
            a[rows(i), :] = value
            at[:, rows(i)] = value.T

    def piece_hidden(half):
        wait_weights(half)

        @pl.loop(0, T // B)
        def _(i):
            here = a[rows(i), :]
            gate = nn(here, wgv[half])
            up = nn(here, wuv[half])
            dact = nt(ct[rows(i), :], wdv[half]).astype(BF).astype(F32)
            sig = jax.nn.sigmoid(gate)
            silu = gate * sig
            actt[:, rows(i)] = (silu * up).astype(BF).T
            dup[rows(i), :] = (dact * silu).astype(BF)
            dgate[rows(i), :] = (dact * up * (sig * (1.0 + gate * (1.0 - sig)))).astype(BF)

    def piece_gate_up(jj, half):
        slot = 3 * (jj % 2) + half
        for mat, z in enumerate((dgate, dup)):
            for n in range(2):
                term = nn(at[pl.ds(n * 384, 384), :], z[...]).astype(BF)
                for i in range(4):
                    d = 4 * n + i
                    grad[slot, d % 2, d // 2, pl.ds(96 * mat, 96), :] = term[96 * i : 96 * (i + 1)]

    def piece_down(jj, half):
        slot = 3 * (jj % 2) + 2
        for n in range(2):
            term = nn(actt[pl.ds(n * 256, 256), :], ct[...]).astype(BF)
            for i in range(2):
                d = 4 * half + 2 * n + i
                block = term[128 * i : 128 * (i + 1)]
                grad[slot, d % 2, d // 2, pl.ds(0, 128), :] = block[:, :512]
                grad[slot, d % 2, d // 2, pl.ds(128, 64), pl.ds(0, 256)] = block[:64, 512:]
                grad[slot, d % 2, d // 2, pl.ds(128, 64), pl.ds(256, 256)] = block[64:, 512:]

        @pl.when(jj < 3)
        def _():
            @pl.loop(0, T // B)
            def _(i):
                acc[rows(i), :] += nt(dgate[rows(i), :], wgv[half]) + nt(dup[rows(i), :], wuv[half])

    def next_layer():
        @pl.loop(0, T // B)
        def _(i):
            wide = h[rows(i), :].astype(F32)
            scale = scale_of(wide)
            da = acc[rows(i), :].astype(BF).astype(F32)
            dot = jnp.mean(da * wide, -1, keepdims=True)
            dh = (da * scale - wide * (scale * scale * scale * dot)).astype(BF)
            ct[rows(i), :] = ct[rows(i), :] + dh

        load = pltpu.make_async_copy(x_hbm, h, load_sem.at[0])
        load.start()
        load.wait()
        norm_states()

    def start_forward(block, half):
        ff = pl.ds(pl.multiple_of(block * S, S), S)
        pltpu.make_async_copy(wg_hbm.at[0, :, ff], wgv.at[half], weight_sem.at[half, 0]).start()
        pltpu.make_async_copy(wu_hbm.at[0, :, ff], wuv.at[half], weight_sem.at[half, 1]).start()
        pltpu.make_async_copy(wd_hbm.at[0, ff, :], wdv.at[half], weight_sem.at[half, 2]).start()

    def piece_forward(half):
        wait_weights(half)

        @pl.loop(0, T // B)
        def _(i):
            here = a[rows(i), :]
            gate = nn(here, wgv[half])
            up = nn(here, wuv[half])
            act = (gate * jax.nn.sigmoid(gate) * up).astype(BF)
            acc[rows(i), :] += nn(act, wdv[half])

    loads = [pltpu.make_async_copy(x_hbm, h, load_sem.at[0]), pltpu.make_async_copy(dy_hbm, ct, load_sem.at[1])]
    loads[0].start()
    start_forward(0, 0)
    loads[1].start()
    barrier = pltpu.get_barrier_semaphore()
    for device in (partner, xn, yn):
        pl.semaphore_signal(barrier, inc=1, device_id=(rep, device), device_id_type=pl.DeviceIdType.MESH)
    loads[0].wait()

    @pl.loop(0, T // B)
    def _(i):
        wide = h[rows(i), :].astype(F32)
        a[rows(i), :] = (wide * scale_of(wide)).astype(BF)
        acc[rows(i), :] = jnp.zeros((B, D), F32)

    @pl.loop(0, FF // S // 2)
    def _(pair):
        start_forward(2 * pair + 1, 1)
        piece_forward(0)

        @pl.when(pair < FF // S // 2 - 1)
        def _():
            start_forward(2 * pair + 2, 0)

        @pl.when(pair == FF // S // 2 - 1)
        def _():
            start_weights(0, 0)

        piece_forward(1)

    @pl.loop(0, T // B)
    def _(i):
        h[rows(i), :] = h[rows(i), :] + acc[rows(i), :].astype(BF)
        acc[rows(i), :] = jnp.zeros((B, D), F32)

    norm_states()
    loads[1].wait()
    pl.semaphore_wait(barrier, 3)

    @pl.loop(0, 8)
    def _(jj):
        @pl.when(jj == 3)
        def _():
            next_layer()

        for half in range(2):

            @pl.when(jj < 6)
            def _():
                if half == 0:
                    start_weights(jj, 1)
                else:

                    @pl.when(jj < 5)
                    def _():
                        start_weights(jj + 1, 0)

                piece_hidden(half)

            tick(jj, 3 * half)

            @pl.when(jj < 6)
            def _():
                piece_gate_up(jj, half)

            tick(jj, 3 * half + 1)

            @pl.when(jj < 6)
            def _():
                piece_down(jj, half)

            tick(jj, 3 * half + 2)


def train_step(x, dy, *arrays):
    anywhere = pl.BlockSpec(memory_space=pl.ANY)
    block = (R, S)
    return pl.pallas_call(
        step_kernel,
        out_shape=(
            jax.ShapeDtypeStruct((UNITS, 2, 4) + block, BF),
            jax.ShapeDtypeStruct((UNITS,) + block, BF),
        ),
        in_specs=[anywhere] * 11,
        out_specs=(anywhere, anywhere),
        scratch_shapes=[
            pltpu.VMEM((T, D), BF),
            pltpu.VMEM((T, D), BF),
            pltpu.VMEM((D, T), BF),
            pltpu.VMEM((T, D), BF),
            pltpu.VMEM((T, D), F32),
            pltpu.VMEM((2, D, S), BF),
            pltpu.VMEM((2, D, S), BF),
            pltpu.VMEM((2, S, D), BF),
            pltpu.VMEM((S, T), BF),
            pltpu.VMEM((T, S), BF),
            pltpu.VMEM((T, S), BF),
            pltpu.VMEM((NS, 2, 4) + block, BF),
            pltpu.VMEM((NS, 4) + block, BF),
            pltpu.VMEM((NS, 2, R // 2, S), BF),
            pltpu.VMEM((NS, 2) + block, BF),
            pltpu.VMEM((3,) + block, F32),
            pltpu.VMEM((3,) + block, F32),
            pltpu.VMEM((3,) + block, BF),
            pltpu.VMEM((NS,) + block, BF),
            pltpu.VMEM((NS,) + block, BF),
            pltpu.SemaphoreType.DMA((KINDS, NS)),
            pltpu.SemaphoreType.DMA((KINDS, NS)),
            pltpu.SemaphoreType.DMA((2,)),
            pltpu.SemaphoreType.DMA((2, 3)),
            pltpu.SemaphoreType.DMA((3, 3)),
            pltpu.SemaphoreType.DMA((2, NS)),
        ],
        compiler_params=pltpu.CompilerParams(
            collective_id=0, has_side_effects=True, vmem_limit_bytes=VMEM_LIMIT
        ),
        name="train_step",
    )(x, dy, *arrays)


def unpack_kernel(
    w_hbm, g_hbm, mg, mu, md, vg, vu, vd,
    gate, up, down, new_mg, new_mu, new_md, new_vg, new_vu, new_vd,
    held, g_ref, wide, tall, out_wide, out_tall, held_sem, g_sem, load_sem, out_sem, store_sem,
):
    wides, talls = (mg, mu, vg, vu), (md, vd)
    new_wides, new_talls = (new_mg, new_mu, new_vg, new_vu), (new_md, new_vd)

    def load_block(n):
        return pltpu.make_async_copy(w_hbm.at[1 - n // 8, :, n % 2, (n % 8) // 2], held.at[n], held_sem.at[n])

    def load_layer(layer):
        copies = [pltpu.make_async_copy(g_hbm.at[1 - layer], g_ref.at[layer], g_sem.at[layer])]
        for i, ref in enumerate(wides):
            copies.append(pltpu.make_async_copy(ref.at[layer], wide.at[i, layer], load_sem.at[layer, i]))
        for i, ref in enumerate(talls):
            copies.append(pltpu.make_async_copy(ref.at[layer], tall.at[i, layer], load_sem.at[layer, 4 + i]))
        return copies

    def stores(n):
        layer, d, slot = n // 8, n % 8, n % 4
        few, many = pl.ds(pl.multiple_of(d * 96, 32), 96), pl.ds(pl.multiple_of(d * 384, 128), 384)
        return (
            pltpu.make_async_copy(out_wide.at[slot, 0], gate.at[layer, few], out_sem.at[slot, 0]),
            pltpu.make_async_copy(out_wide.at[slot, 1], up.at[layer, few], out_sem.at[slot, 1]),
            pltpu.make_async_copy(out_tall.at[slot], down.at[layer, many], out_sem.at[slot, 2]),
        )

    def moments(g, m_ref, v_ref, at):
        g = g.astype(F32)
        m_ref[at] = 0.9 * m_ref[at] + 0.1 * g
        v_ref[at] = 0.95 * v_ref[at] + 0.05 * g * g

    load_block(0).start()
    load_block(1).start()
    for copy in load_layer(0):
        copy.start()

    @pl.loop(2, 8)
    def _(n):
        load_block(n).start()

    for copy in load_layer(1):
        copy.start()

    @pl.loop(8, 16)
    def _(n):
        load_block(n).start()

    @pl.loop(0, 16)
    def _(n):
        layer, d, slot = n // 8, n % 8, n % 4

        @pl.when(n >= 4)
        def _():
            for copy in stores(n - 4):
                copy.wait()

        load_block(n).wait()
        for j in range(3):
            for half in range(2):
                for i in range(4):
                    to = pl.ds((4 * half + i) * 384 + j * 128, 128)
                    out_wide[slot, 0, :, to] = held[n, 3 * j + half, :96, i * 128 : (i + 1) * 128]
                    out_wide[slot, 1, :, to] = held[n, 3 * j + half, 96:, i * 128 : (i + 1) * 128]
            out_tall[slot, pl.ds(j * 128, 128), :512] = held[n, 3 * j + 2, :128, :]
            out_tall[slot, pl.ds(j * 128, 64), 512:] = held[n, 3 * j + 2, 128:, :256]
            out_tall[slot, pl.ds(j * 128 + 64, 64), 512:] = held[n, 3 * j + 2, 128:, 256:]
        for copy in stores(n):
            copy.start()

        for first in range(2):

            @pl.when(n == 8 * first)
            def _():
                for copy in load_layer(first):
                    copy.wait()

        lanes = pl.ds(pl.multiple_of((d % 4) * 128, 128), 128)
        block = pl.ds(pl.multiple_of(d * 384, 128), 384)
        for mat in range(2):
            for j in range(3):
                at = (layer, slice(None), pl.ds(pl.multiple_of(d * 384 + j * 128, 128), 128))
                g = g_ref[layer, 3 * j + d // 4, 96 * mat : 96 * (mat + 1), lanes]
                moments(g, wide.at[mat], wide.at[2 + mat], at)
        for i, ref in enumerate(new_wides):
            pltpu.make_async_copy(wide.at[i, layer, :, block], ref.at[layer, :, block], store_sem.at[i]).start()

        @pl.when(d < 3)
        def _():
            rows = pl.ds(pl.multiple_of(d * 128, 128), 128)
            for row, count, col, width, to_row, to_col in ((0, 128, 0, 512, 0, 0), (128, 64, 0, 256, 0, 512), (128, 64, 256, 256, 64, 512)):
                g = g_ref[layer, 3 * d + 2, row : row + count, col : col + width]
                at = (layer, pl.ds(pl.multiple_of(d * 128 + to_row, 64), count), slice(to_col, to_col + width))
                moments(g, tall.at[0], tall.at[1], at)
            for i, ref in enumerate(new_talls):
                pltpu.make_async_copy(tall.at[i, layer, rows], ref.at[layer, rows], store_sem.at[4 + i]).start()

    @pl.loop(12, 16)
    def _(n):
        for copy in stores(n):
            copy.wait()

    for i, ref in enumerate(new_wides):
        pltpu.make_async_copy(wide.at[i], ref, store_sem.at[i]).wait()
    for i, ref in enumerate(new_talls):
        pltpu.make_async_copy(tall.at[i], ref, store_sem.at[4 + i]).wait()


def unpack(wout, gout, *moments):
    anywhere = pl.BlockSpec(memory_space=pl.ANY)
    return pl.pallas_call(
        unpack_kernel,
        out_shape=[jax.ShapeDtypeStruct(s, BF) for s in ((2, D, FF), (2, D, FF), (2, FF, D))]
        + [jax.ShapeDtypeStruct(m.shape, F32) for m in moments],
        in_specs=[anywhere] * 8,
        out_specs=[anywhere] * 9,
        scratch_shapes=[
            pltpu.VMEM((16, 9, R, S), BF),
            pltpu.VMEM((2, 9, R, S), BF),
            pltpu.VMEM((4, 2, 96, FF), F32),
            pltpu.VMEM((2, 2, 384, D), F32),
            pltpu.VMEM((4, 2, 96, FF), BF),
            pltpu.VMEM((4, 384, D), BF),
            pltpu.SemaphoreType.DMA((16,)),
            pltpu.SemaphoreType.DMA((2,)),
            pltpu.SemaphoreType.DMA((2, 6)),
            pltpu.SemaphoreType.DMA((4, 3)),
            pltpu.SemaphoreType.DMA((6,)),
        ],
        compiler_params=pltpu.CompilerParams(vmem_limit_bytes=VMEM_LIMIT),
        name="unpack",
    )(wout.reshape(2, 9, 2, 4, R, S), gout.reshape(2, 9, R, S), *moments)


def solution(mesh):
    def body(x, dy, wg, wu, wd, mg, mu, md, vg, vu, vd):
        wout, gout = train_step(x[0], dy[0], wg, wu, wd, mg, mu, md, vg, vu, vd)
        return tuple(unpack(wout, gout, mg, mu, md, vg, vu, vd))

    tok, whole, rows = P(("rep", "dp")), P(), P(None, "dp")
    return jax.shard_map(
        body,
        mesh=mesh,
        in_specs=(tok, tok) + (whole,) * 3 + (rows,) * 6,
        out_specs=(P("rep"),) * 3 + (P("rep", "dp"),) * 6,
        check_vma=False,
    )
```

```python
import jax
import jax.numpy as jnp
from jax import lax
from jax.experimental import pallas as pl
from jax.experimental.pallas import tpu as pltpu
from jax.sharding import PartitionSpec as P

T, D, FF = 2048, 768, 3072
S = 512
B = 512
TICKS = 8
R = 192
NS = 6
LAGS = (0, 1, 3, 5, 7, 10, 11)
UNITS = 18
VMEM_LIMIT = 66_500_000
BF, F32 = jnp.bfloat16, jnp.float32


def nn(a, b):
    return jnp.dot(a, b, preferred_element_type=F32)


def nt(a, b):
    return lax.dot_general(a, b, (((1,), (1,)), ((), ())), preferred_element_type=F32)


def scale_of(wide):
    return lax.rsqrt(jnp.mean(wide * wide, -1, keepdims=True) + 1e-6)


S0, S1X, S1Y, S2X, S2Y, G1X, G1Y, G1P, G2X, G2Y, FX, FY, FD = range(13)
KINDS = 13


def step_kernel(
    x_hbm, dy_hbm, wg_hbm, wu_hbm, wd_hbm, mg_hbm, mu_hbm, md_hbm, vg_hbm, vu_hbm, vd_hbm,
    wout, gout,
    h, a, at, ct, acc, wgv, wuv, wdv, actt, dgate, dup,
    grad, recv0, recv1, recv2, mbuf, vbuf, wbuf, wnew, gbuf,
    send_sem, recv_sem, load_sem, weight_sem, moment_sem, out_sem,
):
    rep, me = lax.axis_index("rep"), lax.axis_index("dp")
    c, qm = me % 2, me // 2
    qx, qy = (qm + 2) % 4, qm + 1 - 2 * (qm % 2)
    qd = (qy + 2) % 4
    partner, xn, yn = 2 * qm + 1 - c, 2 * qx + c, 2 * qy + c

    def remote(src, dst, kind, slot, device):
        return pltpu.make_async_remote_copy(
            src_ref=src, dst_ref=dst, send_sem=send_sem.at[kind, slot], recv_sem=recv_sem.at[kind, slot],
            device_id=(rep, device), device_id_type=pl.DeviceIdType.MESH,
        )

    half_p, half_q = pl.ds(0, R // 2), pl.ds(R // 2, R // 2)

    def copy_of(kind, u, slot):
        if kind == S0:
            return remote(grad.at[slot, 1 - c], recv0.at[slot], kind, slot, partner)
        if kind == S1X:
            return remote(grad.at[slot, c, qd, half_p], recv1.at[slot, 0], kind, slot, xn)
        if kind == S1Y:
            return remote(grad.at[slot, c, qd, half_q], recv1.at[slot, 1], kind, slot, yn)
        if kind == S2X:
            return remote(grad.at[slot, c, qx], recv2.at[slot, 0], kind, slot, xn)
        if kind == S2Y:
            return remote(grad.at[slot, c, qy], recv2.at[slot, 1], kind, slot, yn)
        if kind in (G1X, G1Y, G1P):
            to = {G1X: xn, G1Y: yn, G1P: partner}[kind]
            return remote(wnew.at[slot], wout.at[u, c, qm], kind, slot, to)
        if kind == G2X:
            return remote(wout.at[u, c, qy, half_p], wout.at[u, c, qy, half_p], kind, slot, xn)
        if kind == G2Y:
            return remote(wout.at[u, c, qx, half_q], wout.at[u, c, qx, half_q], kind, slot, yn)
        q = {FX: qx, FY: qy, FD: qd}[kind]
        return remote(wout.at[u, c, q], wout.at[u, c, q], kind, slot, partner)

    def own_copies(u, slot):
        return (
            pltpu.make_async_copy(wnew.at[slot], wout.at[u, c, qm], out_sem.at[0, slot]),
            pltpu.make_async_copy(gbuf.at[slot], gout.at[u], out_sem.at[1, slot]),
        )

    def rows(i):
        return pl.ds(pl.multiple_of(i * B, B), B)

    def start_weights(jj, half):
        layer, j = 1 - jj // 3, jj % 3
        for i in range(4):
            ff = pl.ds(pl.multiple_of((4 * half + i) * 384 + j * 128, 128), 128)
            here = pl.ds(i * 128, 128)
            pltpu.make_async_copy(wg_hbm.at[layer, :, ff], wgv.at[half, :, here], weight_sem.at[half, 0]).start()
            pltpu.make_async_copy(wu_hbm.at[layer, :, ff], wuv.at[half, :, here], weight_sem.at[half, 1]).start()
            pltpu.make_async_copy(wd_hbm.at[layer, ff, :], wdv.at[half, here, :], weight_sem.at[half, 2]).start()

    def wait_weights(half):
        pltpu.make_async_copy(wgv.at[half], wgv.at[half], weight_sem.at[half, 0]).wait()
        pltpu.make_async_copy(wuv.at[half], wuv.at[half], weight_sem.at[half, 1]).wait()
        pltpu.make_async_copy(wdv.at[half], wdv.at[half], weight_sem.at[half, 2]).wait()

    def start_moments(jj, k):
        layer, j = 1 - jj // 3, jj % 3
        mine = pl.ds(pl.multiple_of(me * 96, 32), 96)
        for n, (bufs, refs) in enumerate(
            ((mbuf, (mg_hbm, mu_hbm, md_hbm)), (vbuf, (vg_hbm, vu_hbm, vd_hbm)), (wbuf, (wg_hbm, wu_hbm, wd_hbm)))
        ):
            sem = moment_sem.at[k, n]
            if k < 2:
                for mat in range(2):
                    for i in range(4):
                        ff = pl.ds(pl.multiple_of((4 * k + i) * 384 + j * 128, 128), 128)
                        src = refs[mat].at[layer, mine if n == 2 else slice(None), ff]
                        pltpu.make_async_copy(src, bufs.at[k, pl.ds(96 * mat, 96), pl.ds(128 * i, 128)], sem).start()
            else:
                first = j * 128 if n < 2 else me * 384 + j * 128
                for row, count, col, width, to_row, to_col in (
                    (0, 128, 0, 512, 0, 0),
                    (0, 64, 512, 256, 128, 0),
                    (64, 64, 512, 256, 128, 256),
                ):
                    src = refs[2].at[layer, pl.ds(pl.multiple_of(first + row, 64), count), pl.ds(col, width)]
                    pltpu.make_async_copy(src, bufs.at[k, pl.ds(to_row, count), pl.ds(to_col, width)], sem).start()

    def wait_moments(k):
        for n, bufs in enumerate((mbuf, vbuf, wbuf)):
            pltpu.make_async_copy(bufs.at[k], bufs.at[k], moment_sem.at[k, n]).wait()

    def f32(ref_value):
        return ref_value.astype(F32)

    def gather_stage(stage, jj, k):
        u, slot = 3 * jj + k, 3 * (jj % 2) + k
        top, low = slice(0, R // 2), slice(R // 2, R)
        if stage == 1:
            copy_of(S0, u, slot).wait_recv()
            grad[slot, c, qd] = (f32(grad[slot, c, qd]) + f32(recv0[slot, qd])).astype(BF)
        if stage == 2:
            start_moments(jj, k)
            copy_of(S1X, u, slot).wait_recv()
            copy_of(S1Y, u, slot).wait_recv()
            for q, with_p in ((qy, True), (qx, False)):
                for part, is_p in ((top, True), (low, False)):
                    total = f32(grad[slot, c, q, part]) + f32(recv0[slot, q, part])
                    if is_p and with_p:
                        total += f32(recv1[slot, 0])
                    if not is_p and not with_p:
                        total += f32(recv1[slot, 1])
                    grad[slot, c, q, part] = total.astype(BF)
        if stage == 3:
            wait_moments(k)
            copy_of(S2X, u, slot).wait_recv()
            copy_of(S2Y, u, slot).wait_recv()
            for part in (top, low):
                g = f32(grad[slot, c, qm, part]) + f32(recv0[slot, qm, part])
                g = (g + f32(recv2[slot, 0, part]) + f32(recv2[slot, 1, part])).astype(BF)
                gbuf[slot, part] = g
                g = g.astype(F32)
                m = 0.9 * mbuf[k, part] + 0.1 * g
                v = 0.95 * vbuf[k, part] + 0.05 * g * g
                w = f32(wbuf[k, part])
                wnew[slot, part] = (w - 0.02 * (m * lax.rsqrt(v + 1e-8) + 0.1 * w)).astype(BF)
            for kind in (S0, S1X, S1Y, S2X, S2Y):
                copy_of(kind, u, slot).wait_send()

    def send_stage(stage, jj, k):
        u, slot = 3 * jj + k, 3 * (jj % 2) + k
        if stage == 1:
            copy_of(S1X, u, slot).start()
            copy_of(S1Y, u, slot).start()
        if stage == 2:
            copy_of(S2X, u, slot).start()
            copy_of(S2Y, u, slot).start()
        if stage == 3:
            for kind in (G1X, G1Y, G1P):
                copy_of(kind, u, slot).start()
            for copy in own_copies(u, slot):
                copy.start()
        if stage == 4:
            copy_of(G1X, u, slot).wait_recv()
            copy_of(G1Y, u, slot).wait_recv()
            for kind in (G2X, G2Y, FX, FY):
                copy_of(kind, u, slot).start()
        if stage == 5:
            copy_of(G2X, u, slot).wait_recv()
            copy_of(G2Y, u, slot).wait_recv()
            copy_of(FD, u, slot).start()
        if stage == 6:
            for kind in (G1P, FX, FY, FD):
                copy_of(kind, u, slot).wait_recv()
            for kind in (G1X, G1Y, G1P, G2X, G2Y, FX, FY, FD):
                copy_of(kind, u, slot).wait_send()
            for copy in own_copies(u, slot):
                copy.wait()

    def tick(jj, p):
        active = []
        for stage in range(1, 7):
            q, r = divmod(p - LAGS[stage], TICKS)
            if r in (1, 4, 5):
                active.append((stage, jj + q, {1: 0, 4: 1, 5: 2}[r]))
        for stage, unit_jj, k in active:
            if stage <= 3:

                @pl.when((unit_jj >= 0) & (unit_jj < 6))
                def _():
                    gather_stage(stage, unit_jj, k)

        if p in (1, 4, 5):

            @pl.when(jj < 6)
            def _():
                k = {1: 0, 4: 1, 5: 2}[p]
                copy_of(S0, 3 * jj + k, 3 * (jj % 2) + k).start()

        for stage, unit_jj, k in active:

            @pl.when((unit_jj >= 0) & (unit_jj < 6))
            def _():
                send_stage(stage, unit_jj, k)

    def norm_states():
        @pl.loop(0, T // B)
        def _(i):
            wide = h[rows(i), :].astype(F32)
            value = (wide * scale_of(wide)).astype(BF)
            a[rows(i), :] = value
            at[:, rows(i)] = value.T

    def piece_hidden(half):
        wait_weights(half)

        @pl.loop(0, T // B)
        def _(i):
            here = a[rows(i), :]
            gate = nn(here, wgv[half])
            up = nn(here, wuv[half])
            dact = nt(ct[rows(i), :], wdv[half]).astype(BF).astype(F32)
            sig = jax.nn.sigmoid(gate)
            silu = gate * sig
            actt[:, rows(i)] = (silu * up).astype(BF).T
            dup[half, rows(i), :] = (dact * silu).astype(BF)
            dgate[half, rows(i), :] = (dact * up * (sig * (1.0 + gate * (1.0 - sig)))).astype(BF)

    def piece_gate_up(jj, half):
        slot = 3 * (jj % 2) + half
        for mat, z in enumerate((dgate, dup)):
            for n in range(2):
                term = nn(at[pl.ds(n * 384, 384), :], z[half]).astype(BF)
                for i in range(4):
                    d = 4 * n + i
                    grad[slot, d % 2, d // 2, pl.ds(96 * mat, 96), :] = term[96 * i : 96 * (i + 1)]

    def piece_down(jj, half):
        slot = 3 * (jj % 2) + 2
        for n in range(2):
            term = nn(actt[pl.ds(n * 256, 256), :], ct[...]).astype(BF)
            for i in range(2):
                d = 4 * half + 2 * n + i
                block = term[128 * i : 128 * (i + 1)]
                grad[slot, d % 2, d // 2, pl.ds(0, 128), :] = block[:, :512]
                grad[slot, d % 2, d // 2, pl.ds(128, 64), pl.ds(0, 256)] = block[:64, 512:]
                grad[slot, d % 2, d // 2, pl.ds(128, 64), pl.ds(256, 256)] = block[64:, 512:]

    def piece_states(half):
        @pl.loop(0, T // B)
        def _(i):
            acc[rows(i), :] += nt(dgate[half, rows(i), :], wgv[half]) + nt(dup[half, rows(i), :], wuv[half])

    def next_layer():
        @pl.loop(0, T // B)
        def _(i):
            wide = h[rows(i), :].astype(F32)
            scale = scale_of(wide)
            da = acc[rows(i), :].astype(BF).astype(F32)
            dot = jnp.mean(da * wide, -1, keepdims=True)
            dh = (da * scale - wide * (scale * scale * scale * dot)).astype(BF)
            ct[rows(i), :] = ct[rows(i), :] + dh
            pltpu.make_async_copy(x_hbm.at[rows(i)], h.at[rows(i)], load_sem.at[0]).start()

        pltpu.make_async_copy(x_hbm, h, load_sem.at[0]).wait()
        norm_states()

    def start_forward(block, half):
        ff = pl.ds(pl.multiple_of(block * S, S), S)
        pltpu.make_async_copy(wg_hbm.at[0, :, ff], wgv.at[half], weight_sem.at[half, 0]).start()
        pltpu.make_async_copy(wu_hbm.at[0, :, ff], wuv.at[half], weight_sem.at[half, 1]).start()
        pltpu.make_async_copy(wd_hbm.at[0, ff, :], wdv.at[half], weight_sem.at[half, 2]).start()

    def piece_forward(half):
        wait_weights(half)

        @pl.loop(0, T // B)
        def _(i):
            here = a[rows(i), :]
            gate = nn(here, wgv[half])
            up = nn(here, wuv[half])
            act = (gate * jax.nn.sigmoid(gate) * up).astype(BF)
            acc[rows(i), :] += nn(act, wdv[half])

    loads = [pltpu.make_async_copy(x_hbm, h, load_sem.at[0]), pltpu.make_async_copy(dy_hbm, ct, load_sem.at[1])]
    loads[0].start()
    start_forward(0, 0)
    loads[1].start()
    barrier = pltpu.get_barrier_semaphore()
    for device in (partner, xn, yn):
        pl.semaphore_signal(barrier, inc=1, device_id=(rep, device), device_id_type=pl.DeviceIdType.MESH)
    loads[0].wait()

    @pl.loop(0, T // B)
    def _(i):
        wide = h[rows(i), :].astype(F32)
        a[rows(i), :] = (wide * scale_of(wide)).astype(BF)
        acc[rows(i), :] = jnp.zeros((B, D), F32)

    @pl.loop(0, FF // S // 2)
    def _(pair):
        start_forward(2 * pair + 1, 1)
        piece_forward(0)

        @pl.when(pair < FF // S // 2 - 1)
        def _():
            start_forward(2 * pair + 2, 0)

        @pl.when(pair == FF // S // 2 - 1)
        def _():
            start_weights(0, 0)

        piece_forward(1)

    @pl.loop(0, T // B)
    def _(i):
        h[rows(i), :] = h[rows(i), :] + acc[rows(i), :].astype(BF)
        acc[rows(i), :] = jnp.zeros((B, D), F32)

    norm_states()
    loads[1].wait()
    pl.semaphore_wait(barrier, 3)

    @pl.loop(0, 8)
    def _(jj):
        @pl.when(jj == 3)
        def _():
            next_layer()

        for half in range(2):

            @pl.when(jj < 6)
            def _():
                if half == 0:
                    start_weights(jj, 1)
                piece_hidden(half)

            tick(jj, 3 * half)

            @pl.when(jj < 6)
            def _():
                piece_gate_up(jj, half)

            tick(jj, 3 * half + 1)

            @pl.when(jj < 6)
            def _():
                piece_down(jj, half)

            tick(jj, 3 * half + 2)

        for half in range(2):

            @pl.when(jj < 3)
            def _():
                piece_states(half)

            if half == 0:

                @pl.when(jj < 5)
                def _():
                    start_weights(jj + 1, 0)

            tick(jj, 6 + half)


def train_step(x, dy, *arrays):
    anywhere = pl.BlockSpec(memory_space=pl.ANY)
    block = (R, S)
    return pl.pallas_call(
        step_kernel,
        out_shape=(
            jax.ShapeDtypeStruct((UNITS, 2, 4) + block, BF),
            jax.ShapeDtypeStruct((UNITS,) + block, BF),
        ),
        in_specs=[anywhere] * 11,
        out_specs=(anywhere, anywhere),
        scratch_shapes=[
            pltpu.VMEM((T, D), BF),
            pltpu.VMEM((T, D), BF),
            pltpu.VMEM((D, T), BF),
            pltpu.VMEM((T, D), BF),
            pltpu.VMEM((T, D), F32),
            pltpu.VMEM((2, D, S), BF),
            pltpu.VMEM((2, D, S), BF),
            pltpu.VMEM((2, S, D), BF),
            pltpu.VMEM((S, T), BF),
            pltpu.VMEM((2, T, S), BF),
            pltpu.VMEM((2, T, S), BF),
            pltpu.VMEM((NS, 2, 4) + block, BF),
            pltpu.VMEM((NS, 4) + block, BF),
            pltpu.VMEM((NS, 2, R // 2, S), BF),
            pltpu.VMEM((NS, 2) + block, BF),
            pltpu.VMEM((3,) + block, F32),
            pltpu.VMEM((3,) + block, F32),
            pltpu.VMEM((3,) + block, BF),
            pltpu.VMEM((NS,) + block, BF),
            pltpu.VMEM((NS,) + block, BF),
            pltpu.SemaphoreType.DMA((KINDS, NS)),
            pltpu.SemaphoreType.DMA((KINDS, NS)),
            pltpu.SemaphoreType.DMA((2,)),
            pltpu.SemaphoreType.DMA((2, 3)),
            pltpu.SemaphoreType.DMA((3, 3)),
            pltpu.SemaphoreType.DMA((2, NS)),
        ],
        compiler_params=pltpu.CompilerParams(
            collective_id=0, has_side_effects=True, vmem_limit_bytes=VMEM_LIMIT
        ),
        name="train_step",
    )(x, dy, *arrays)


def unpack_kernel(
    w_hbm, g_hbm, mg, mu, md, vg, vu, vd,
    gate, up, down, new_mg, new_mu, new_md, new_vg, new_vu, new_vd,
    held, g_ref, wide, tall, out_wide, out_tall, held_sem, g_sem, load_sem, out_sem, store_sem,
):
    wides, talls = (mg, mu, vg, vu), (md, vd)
    new_wides, new_talls = (new_mg, new_mu, new_vg, new_vu), (new_md, new_vd)

    def load_block(n):
        return pltpu.make_async_copy(w_hbm.at[1 - n // 8, :, n % 2, (n % 8) // 2], held.at[n], held_sem.at[n])

    def load_layer(layer):
        copies = [pltpu.make_async_copy(g_hbm.at[1 - layer], g_ref.at[layer], g_sem.at[layer])]
        for i, ref in enumerate(wides):
            copies.append(pltpu.make_async_copy(ref.at[layer], wide.at[i, layer], load_sem.at[layer, i]))
        for i, ref in enumerate(talls):
            copies.append(pltpu.make_async_copy(ref.at[layer], tall.at[i, layer], load_sem.at[layer, 4 + i]))
        return copies

    def stores(n):
        layer, d, slot = n // 8, n % 8, n % 4
        few, many = pl.ds(pl.multiple_of(d * 96, 32), 96), pl.ds(pl.multiple_of(d * 384, 128), 384)
        return (
            pltpu.make_async_copy(out_wide.at[slot, 0], gate.at[layer, few], out_sem.at[slot, 0]),
            pltpu.make_async_copy(out_wide.at[slot, 1], up.at[layer, few], out_sem.at[slot, 1]),
            pltpu.make_async_copy(out_tall.at[slot], down.at[layer, many], out_sem.at[slot, 2]),
        )

    def moments(g, m_ref, v_ref, at):
        g = g.astype(F32)
        m_ref[at] = 0.9 * m_ref[at] + 0.1 * g
        v_ref[at] = 0.95 * v_ref[at] + 0.05 * g * g

    load_block(0).start()
    load_block(1).start()
    for copy in load_layer(0):
        copy.start()

    @pl.loop(2, 8)
    def _(n):
        load_block(n).start()

    for copy in load_layer(1):
        copy.start()

    @pl.loop(8, 16)
    def _(n):
        load_block(n).start()

    @pl.loop(0, 16)
    def _(n):
        layer, d, slot = n // 8, n % 8, n % 4

        @pl.when(n >= 4)
        def _():
            for copy in stores(n - 4):
                copy.wait()

        load_block(n).wait()
        for j in range(3):
            for half in range(2):
                for i in range(4):
                    to = pl.ds((4 * half + i) * 384 + j * 128, 128)
                    out_wide[slot, 0, :, to] = held[n, 3 * j + half, :96, i * 128 : (i + 1) * 128]
                    out_wide[slot, 1, :, to] = held[n, 3 * j + half, 96:, i * 128 : (i + 1) * 128]
            out_tall[slot, pl.ds(j * 128, 128), :512] = held[n, 3 * j + 2, :128, :]
            out_tall[slot, pl.ds(j * 128, 64), 512:] = held[n, 3 * j + 2, 128:, :256]
            out_tall[slot, pl.ds(j * 128 + 64, 64), 512:] = held[n, 3 * j + 2, 128:, 256:]
        for copy in stores(n):
            copy.start()

        for first in range(2):

            @pl.when(n == 8 * first)
            def _():
                for copy in load_layer(first):
                    copy.wait()

        lanes = pl.ds(pl.multiple_of((d % 4) * 128, 128), 128)
        block = pl.ds(pl.multiple_of(d * 384, 128), 384)
        for mat in range(2):
            for j in range(3):
                at = (layer, slice(None), pl.ds(pl.multiple_of(d * 384 + j * 128, 128), 128))
                g = g_ref[layer, 3 * j + d // 4, 96 * mat : 96 * (mat + 1), lanes]
                moments(g, wide.at[mat], wide.at[2 + mat], at)
        for i, ref in enumerate(new_wides):
            pltpu.make_async_copy(wide.at[i, layer, :, block], ref.at[layer, :, block], store_sem.at[i]).start()

        @pl.when(d < 3)
        def _():
            rows = pl.ds(pl.multiple_of(d * 128, 128), 128)
            for row, count, col, width, to_row, to_col in ((0, 128, 0, 512, 0, 0), (128, 64, 0, 256, 0, 512), (128, 64, 256, 256, 64, 512)):
                g = g_ref[layer, 3 * d + 2, row : row + count, col : col + width]
                at = (layer, pl.ds(pl.multiple_of(d * 128 + to_row, 64), count), slice(to_col, to_col + width))
                moments(g, tall.at[0], tall.at[1], at)
            for i, ref in enumerate(new_talls):
                pltpu.make_async_copy(tall.at[i, layer, rows], ref.at[layer, rows], store_sem.at[4 + i]).start()

    @pl.loop(12, 16)
    def _(n):
        for copy in stores(n):
            copy.wait()

    for i, ref in enumerate(new_wides):
        pltpu.make_async_copy(wide.at[i], ref, store_sem.at[i]).wait()
    for i, ref in enumerate(new_talls):
        pltpu.make_async_copy(tall.at[i], ref, store_sem.at[4 + i]).wait()


def unpack(wout, gout, *moments):
    anywhere = pl.BlockSpec(memory_space=pl.ANY)
    return pl.pallas_call(
        unpack_kernel,
        out_shape=[jax.ShapeDtypeStruct(s, BF) for s in ((2, D, FF), (2, D, FF), (2, FF, D))]
        + [jax.ShapeDtypeStruct(m.shape, F32) for m in moments],
        in_specs=[anywhere] * 8,
        out_specs=[anywhere] * 9,
        scratch_shapes=[
            pltpu.VMEM((16, 9, R, S), BF),
            pltpu.VMEM((2, 9, R, S), BF),
            pltpu.VMEM((4, 2, 96, FF), F32),
            pltpu.VMEM((2, 2, 384, D), F32),
            pltpu.VMEM((4, 2, 96, FF), BF),
            pltpu.VMEM((4, 384, D), BF),
            pltpu.SemaphoreType.DMA((16,)),
            pltpu.SemaphoreType.DMA((2,)),
            pltpu.SemaphoreType.DMA((2, 6)),
            pltpu.SemaphoreType.DMA((4, 3)),
            pltpu.SemaphoreType.DMA((6,)),
        ],
        compiler_params=pltpu.CompilerParams(vmem_limit_bytes=VMEM_LIMIT),
        name="unpack",
    )(wout.reshape(2, 9, 2, 4, R, S), gout.reshape(2, 9, R, S), *moments)


def solution(mesh):
    def body(x, dy, wg, wu, wd, mg, mu, md, vg, vu, vd):
        wout, gout = train_step(x[0], dy[0], wg, wu, wd, mg, mu, md, vg, vu, vd)
        return tuple(unpack(wout, gout, mg, mu, md, vg, vu, vd))

    tok, whole, rows = P(("rep", "dp")), P(), P(None, "dp")
    return jax.shard_map(
        body,
        mesh=mesh,
        in_specs=(tok, tok) + (whole,) * 3 + (rows,) * 6,
        out_specs=(P("rep"),) * 3 + (P("rep", "dp"),) * 6,
        check_vma=False,
    )
```

```python
import jax
import jax.numpy as jnp
from jax import lax
from jax.experimental import pallas as pl
from jax.experimental.pallas import tpu as pltpu
from jax.sharding import PartitionSpec as P

T, D, FF = 2048, 768, 3072
S = 512
B = 512
W = 1024
TICKS = 8
R = 192
NS = 6
LAGS = (0, 1, 3, 5, 7, 10, 11)
UNITS = 18
VMEM_LIMIT = 66_500_000
BF, F32 = jnp.bfloat16, jnp.float32


def nn(a, b):
    return jnp.dot(a, b, preferred_element_type=F32)


def nt(a, b):
    return lax.dot_general(a, b, (((1,), (1,)), ((), ())), preferred_element_type=F32)


def scale_of(wide):
    return lax.rsqrt(jnp.mean(wide * wide, -1, keepdims=True) + 1e-6)


S0, S1X, S1Y, S2X, S2Y, G1X, G1Y, G1P, G2X, G2Y, FX, FY, FD = range(13)
KINDS = 13


def step_kernel(
    x_hbm, dy_hbm, wg_hbm, wu_hbm, wd_hbm, mg_hbm, mu_hbm, md_hbm, vg_hbm, vu_hbm, vd_hbm,
    wout, gout,
    h, a, at, ct, acc, wgv, wuv, wdv, actt, dgate, dup,
    grad, recv0, recv1, recv2, mbuf, vbuf, wbuf, wnew, gbuf,
    send_sem, recv_sem, load_sem, weight_sem, moment_sem, out_sem,
):
    rep, me = lax.axis_index("rep"), lax.axis_index("dp")
    c, qm = me % 2, me // 2
    qx, qy = (qm + 2) % 4, qm + 1 - 2 * (qm % 2)
    qd = (qy + 2) % 4
    partner, xn, yn = 2 * qm + 1 - c, 2 * qx + c, 2 * qy + c

    def remote(src, dst, kind, slot, device):
        return pltpu.make_async_remote_copy(
            src_ref=src, dst_ref=dst, send_sem=send_sem.at[kind, slot], recv_sem=recv_sem.at[kind, slot],
            device_id=(rep, device), device_id_type=pl.DeviceIdType.MESH,
        )

    half_p, half_q = pl.ds(0, R // 2), pl.ds(R // 2, R // 2)

    def copy_of(kind, u, slot):
        if kind == S0:
            return remote(grad.at[slot, 1 - c], recv0.at[slot], kind, slot, partner)
        if kind == S1X:
            return remote(grad.at[slot, c, qd, half_p], recv1.at[slot, 0], kind, slot, xn)
        if kind == S1Y:
            return remote(grad.at[slot, c, qd, half_q], recv1.at[slot, 1], kind, slot, yn)
        if kind == S2X:
            return remote(grad.at[slot, c, qx], recv2.at[slot, 0], kind, slot, xn)
        if kind == S2Y:
            return remote(grad.at[slot, c, qy], recv2.at[slot, 1], kind, slot, yn)
        if kind in (G1X, G1Y, G1P):
            to = {G1X: xn, G1Y: yn, G1P: partner}[kind]
            return remote(wnew.at[slot], wout.at[u, c, qm], kind, slot, to)
        if kind == G2X:
            return remote(wout.at[u, c, qy, half_p], wout.at[u, c, qy, half_p], kind, slot, xn)
        if kind == G2Y:
            return remote(wout.at[u, c, qx, half_q], wout.at[u, c, qx, half_q], kind, slot, yn)
        q = {FX: qx, FY: qy, FD: qd}[kind]
        return remote(wout.at[u, c, q], wout.at[u, c, q], kind, slot, partner)

    def own_copies(u, slot):
        return (
            pltpu.make_async_copy(wnew.at[slot], wout.at[u, c, qm], out_sem.at[0, slot]),
            pltpu.make_async_copy(gbuf.at[slot], gout.at[u], out_sem.at[1, slot]),
        )

    def rows(i, size=B):
        return pl.ds(pl.multiple_of(i * size, size), size)

    def start_weights(jj, half):
        layer, j = 1 - jj // 3, jj % 3
        for i in range(4):
            ff = pl.ds(pl.multiple_of((4 * half + i) * 384 + j * 128, 128), 128)
            here = pl.ds(i * 128, 128)
            pltpu.make_async_copy(wg_hbm.at[layer, :, ff], wgv.at[half, :, here], weight_sem.at[half, 0]).start()
            pltpu.make_async_copy(wu_hbm.at[layer, :, ff], wuv.at[half, :, here], weight_sem.at[half, 1]).start()
            pltpu.make_async_copy(wd_hbm.at[layer, ff, :], wdv.at[half, here, :], weight_sem.at[half, 2]).start()

    def wait_weights(half):
        pltpu.make_async_copy(wgv.at[half], wgv.at[half], weight_sem.at[half, 0]).wait()
        pltpu.make_async_copy(wuv.at[half], wuv.at[half], weight_sem.at[half, 1]).wait()
        pltpu.make_async_copy(wdv.at[half], wdv.at[half], weight_sem.at[half, 2]).wait()

    def start_moments(jj, k):
        layer, j = 1 - jj // 3, jj % 3
        mine = pl.ds(pl.multiple_of(me * 96, 32), 96)
        for n, (bufs, refs) in enumerate(
            ((mbuf, (mg_hbm, mu_hbm, md_hbm)), (vbuf, (vg_hbm, vu_hbm, vd_hbm)), (wbuf, (wg_hbm, wu_hbm, wd_hbm)))
        ):
            sem = moment_sem.at[k, n]
            if k < 2:
                for mat in range(2):
                    for i in range(4):
                        ff = pl.ds(pl.multiple_of((4 * k + i) * 384 + j * 128, 128), 128)
                        src = refs[mat].at[layer, mine if n == 2 else slice(None), ff]
                        pltpu.make_async_copy(src, bufs.at[k, pl.ds(96 * mat, 96), pl.ds(128 * i, 128)], sem).start()
            else:
                first = j * 128 if n < 2 else me * 384 + j * 128
                for row, count, col, width, to_row, to_col in (
                    (0, 128, 0, 512, 0, 0),
                    (0, 64, 512, 256, 128, 0),
                    (64, 64, 512, 256, 128, 256),
                ):
                    src = refs[2].at[layer, pl.ds(pl.multiple_of(first + row, 64), count), pl.ds(col, width)]
                    pltpu.make_async_copy(src, bufs.at[k, pl.ds(to_row, count), pl.ds(to_col, width)], sem).start()

    def wait_moments(k):
        for n, bufs in enumerate((mbuf, vbuf, wbuf)):
            pltpu.make_async_copy(bufs.at[k], bufs.at[k], moment_sem.at[k, n]).wait()

    def f32(ref_value):
        return ref_value.astype(F32)

    def gather_stage(stage, jj, k):
        u, slot = 3 * jj + k, 3 * (jj % 2) + k
        top, low = slice(0, R // 2), slice(R // 2, R)
        if stage == 1:
            copy_of(S0, u, slot).wait_recv()
            grad[slot, c, qd] = (f32(grad[slot, c, qd]) + f32(recv0[slot, qd])).astype(BF)
        if stage == 2:
            start_moments(jj, k)
            copy_of(S1X, u, slot).wait_recv()
            copy_of(S1Y, u, slot).wait_recv()
            for q, with_p in ((qy, True), (qx, False)):
                for part, is_p in ((top, True), (low, False)):
                    total = f32(grad[slot, c, q, part]) + f32(recv0[slot, q, part])
                    if is_p and with_p:
                        total += f32(recv1[slot, 0])
                    if not is_p and not with_p:
                        total += f32(recv1[slot, 1])
                    grad[slot, c, q, part] = total.astype(BF)
        if stage == 3:
            wait_moments(k)
            copy_of(S2X, u, slot).wait_recv()
            copy_of(S2Y, u, slot).wait_recv()
            for part in (top, low):
                g = f32(grad[slot, c, qm, part]) + f32(recv0[slot, qm, part])
                g = (g + f32(recv2[slot, 0, part]) + f32(recv2[slot, 1, part])).astype(BF)
                gbuf[slot, part] = g
                g = g.astype(F32)
                m = 0.9 * mbuf[k, part] + 0.1 * g
                v = 0.95 * vbuf[k, part] + 0.05 * g * g
                w = f32(wbuf[k, part])
                wnew[slot, part] = (w - 0.02 * (m * lax.rsqrt(v + 1e-8) + 0.1 * w)).astype(BF)
            for kind in (S0, S1X, S1Y, S2X, S2Y):
                copy_of(kind, u, slot).wait_send()

    def send_stage(stage, jj, k):
        u, slot = 3 * jj + k, 3 * (jj % 2) + k
        if stage == 1:
            copy_of(S1X, u, slot).start()
            copy_of(S1Y, u, slot).start()
        if stage == 2:
            copy_of(S2X, u, slot).start()
            copy_of(S2Y, u, slot).start()
        if stage == 3:
            for kind in (G1X, G1Y, G1P):
                copy_of(kind, u, slot).start()
            for copy in own_copies(u, slot):
                copy.start()
        if stage == 4:
            copy_of(G1X, u, slot).wait_recv()
            copy_of(G1Y, u, slot).wait_recv()
            for kind in (G2X, G2Y, FX, FY):
                copy_of(kind, u, slot).start()
        if stage == 5:
            copy_of(G2X, u, slot).wait_recv()
            copy_of(G2Y, u, slot).wait_recv()
            copy_of(FD, u, slot).start()
        if stage == 6:
            for kind in (G1P, FX, FY, FD):
                copy_of(kind, u, slot).wait_recv()
            for kind in (G1X, G1Y, G1P, G2X, G2Y, FX, FY, FD):
                copy_of(kind, u, slot).wait_send()
            for copy in own_copies(u, slot):
                copy.wait()

    def tick(jj, p):
        active = []
        for stage in range(1, 7):
            q, r = divmod(p - LAGS[stage], TICKS)
            if r in (1, 4, 5):
                active.append((stage, jj + q, {1: 0, 4: 1, 5: 2}[r]))
        for stage, unit_jj, k in active:
            if stage <= 3:

                @pl.when((unit_jj >= 0) & (unit_jj < 6))
                def _():
                    gather_stage(stage, unit_jj, k)

        if p in (1, 4, 5):

            @pl.when(jj < 6)
            def _():
                k = {1: 0, 4: 1, 5: 2}[p]
                copy_of(S0, 3 * jj + k, 3 * (jj % 2) + k).start()

        for stage, unit_jj, k in active:

            @pl.when((unit_jj >= 0) & (unit_jj < 6))
            def _():
                send_stage(stage, unit_jj, k)

    def norm_block(i, states):
        wide = states.astype(F32)
        value = (wide * scale_of(wide)).astype(BF)
        a[rows(i), :] = value
        at[:, rows(i)] = value.T

    def norm_states():
        @pl.loop(0, T // B)
        def _(i):
            norm_block(i, h[rows(i), :])

    def piece_hidden(half):
        wait_weights(half)

        @pl.loop(0, T // W)
        def _(i):
            here = a[rows(i, W), :]
            gate = nn(here, wgv[half])
            up = nn(here, wuv[half])
            dact = nt(ct[rows(i, W), :], wdv[half]).astype(BF).astype(F32)
            sig = jax.nn.sigmoid(gate)
            silu = gate * sig
            actt[:, rows(i, W)] = (silu * up).astype(BF).T
            dup[half, rows(i, W), :] = (dact * silu).astype(BF)
            dgate[half, rows(i, W), :] = (dact * up * (sig * (1.0 + gate * (1.0 - sig)))).astype(BF)

    def piece_gate_up(jj, half):
        slot = 3 * (jj % 2) + half
        for mat, z in enumerate((dgate, dup)):
            for n in range(2):
                term = nn(at[pl.ds(n * 384, 384), :], z[half]).astype(BF)
                for i in range(4):
                    d = 4 * n + i
                    grad[slot, d % 2, d // 2, pl.ds(96 * mat, 96), :] = term[96 * i : 96 * (i + 1)]

    def piece_down(jj, half):
        slot = 3 * (jj % 2) + 2
        for n in range(2):
            term = nn(actt[pl.ds(n * 256, 256), :], ct[...]).astype(BF)
            for i in range(2):
                d = 4 * half + 2 * n + i
                block = term[128 * i : 128 * (i + 1)]
                grad[slot, d % 2, d // 2, pl.ds(0, 128), :] = block[:, :512]
                grad[slot, d % 2, d // 2, pl.ds(128, 64), pl.ds(0, 256)] = block[:64, 512:]
                grad[slot, d % 2, d // 2, pl.ds(128, 64), pl.ds(256, 256)] = block[64:, 512:]

    def piece_states(half):
        @pl.loop(0, T // W)
        def _(i):
            acc[rows(i, W), :] += nt(dgate[half, rows(i, W), :], wgv[half]) + nt(dup[half, rows(i, W), :], wuv[half])

    def next_cotangent():
        @pl.loop(0, T // B)
        def _(i):
            wide = h[rows(i), :].astype(F32)
            scale = scale_of(wide)
            da = acc[rows(i), :].astype(BF).astype(F32)
            dot = jnp.mean(da * wide, -1, keepdims=True)
            dh = (da * scale - wide * (scale * scale * scale * dot)).astype(BF)
            ct[rows(i), :] = ct[rows(i), :] + dh
            pltpu.make_async_copy(x_hbm.at[rows(i)], h.at[rows(i)], load_sem.at[0]).start()

    def next_states():
        pltpu.make_async_copy(x_hbm, h, load_sem.at[0]).wait()
        norm_states()

    def start_forward(block, half):
        ff = pl.ds(pl.multiple_of(block * S, S), S)
        pltpu.make_async_copy(wg_hbm.at[0, :, ff], wgv.at[half], weight_sem.at[half, 0]).start()
        pltpu.make_async_copy(wu_hbm.at[0, :, ff], wuv.at[half], weight_sem.at[half, 1]).start()
        pltpu.make_async_copy(wd_hbm.at[0, ff, :], wdv.at[half], weight_sem.at[half, 2]).start()

    def piece_forward(half):
        wait_weights(half)

        @pl.loop(0, T // W)
        def _(i):
            here = a[rows(i, W), :]
            gate = nn(here, wgv[half])
            up = nn(here, wuv[half])
            act = (gate * jax.nn.sigmoid(gate) * up).astype(BF)
            acc[rows(i, W), :] += nn(act, wdv[half])

    def load_x(i):
        return pltpu.make_async_copy(x_hbm.at[rows(i)], h.at[rows(i)], load_sem.at[1 + i])

    load_dy = pltpu.make_async_copy(dy_hbm, ct, load_sem.at[0])
    for i in range(T // B):
        load_x(i).start()
    start_forward(0, 0)
    load_dy.start()
    barrier = pltpu.get_barrier_semaphore()
    for device in (partner, xn, yn):
        pl.semaphore_signal(barrier, inc=1, device_id=(rep, device), device_id_type=pl.DeviceIdType.MESH)

    @pl.loop(0, T // B)
    def _(i):
        load_x(i).wait()
        wide = h[rows(i), :].astype(F32)
        a[rows(i), :] = (wide * scale_of(wide)).astype(BF)
        acc[rows(i), :] = jnp.zeros((B, D), F32)

    @pl.loop(0, FF // S // 2)
    def _(pair):
        start_forward(2 * pair + 1, 1)
        piece_forward(0)

        @pl.when(pair < FF // S // 2 - 1)
        def _():
            start_forward(2 * pair + 2, 0)

        @pl.when(pair == FF // S // 2 - 1)
        def _():
            start_weights(0, 0)

        piece_forward(1)

    @pl.loop(0, T // B)
    def _(i):
        states = h[rows(i), :] + acc[rows(i), :].astype(BF)
        h[rows(i), :] = states
        acc[rows(i), :] = jnp.zeros((B, D), F32)
        norm_block(i, states)

    load_dy.wait()
    pl.semaphore_wait(barrier, 3)

    @pl.loop(0, 8)
    def _(jj):
        @pl.when(jj == 3)
        def _():
            next_states()

        for half in range(2):

            @pl.when(jj < 6)
            def _():
                if half == 0:
                    start_weights(jj, 1)
                piece_hidden(half)

            tick(jj, 3 * half)

            @pl.when(jj < 6)
            def _():
                piece_gate_up(jj, half)

            tick(jj, 3 * half + 1)

            @pl.when(jj < 6)
            def _():
                piece_down(jj, half)

            tick(jj, 3 * half + 2)

        for half in range(2):

            @pl.when(jj < 3)
            def _():
                piece_states(half)

            if half == 1:

                @pl.when(jj == 2)
                def _():
                    next_cotangent()

            if half == 0:

                @pl.when(jj < 5)
                def _():
                    start_weights(jj + 1, 0)

            tick(jj, 6 + half)


def train_step(x, dy, *arrays):
    anywhere = pl.BlockSpec(memory_space=pl.ANY)
    block = (R, S)
    return pl.pallas_call(
        step_kernel,
        out_shape=(
            jax.ShapeDtypeStruct((UNITS, 2, 4) + block, BF),
            jax.ShapeDtypeStruct((UNITS,) + block, BF),
        ),
        in_specs=[anywhere] * 11,
        out_specs=(anywhere, anywhere),
        scratch_shapes=[
            pltpu.VMEM((T, D), BF),
            pltpu.VMEM((T, D), BF),
            pltpu.VMEM((D, T), BF),
            pltpu.VMEM((T, D), BF),
            pltpu.VMEM((T, D), F32),
            pltpu.VMEM((2, D, S), BF),
            pltpu.VMEM((2, D, S), BF),
            pltpu.VMEM((2, S, D), BF),
            pltpu.VMEM((S, T), BF),
            pltpu.VMEM((2, T, S), BF),
            pltpu.VMEM((2, T, S), BF),
            pltpu.VMEM((NS, 2, 4) + block, BF),
            pltpu.VMEM((NS, 4) + block, BF),
            pltpu.VMEM((NS, 2, R // 2, S), BF),
            pltpu.VMEM((NS, 2) + block, BF),
            pltpu.VMEM((3,) + block, F32),
            pltpu.VMEM((3,) + block, F32),
            pltpu.VMEM((3,) + block, BF),
            pltpu.VMEM((NS,) + block, BF),
            pltpu.VMEM((NS,) + block, BF),
            pltpu.SemaphoreType.DMA((KINDS, NS)),
            pltpu.SemaphoreType.DMA((KINDS, NS)),
            pltpu.SemaphoreType.DMA((1 + T // B,)),
            pltpu.SemaphoreType.DMA((2, 3)),
            pltpu.SemaphoreType.DMA((3, 3)),
            pltpu.SemaphoreType.DMA((2, NS)),
        ],
        compiler_params=pltpu.CompilerParams(
            collective_id=0, has_side_effects=True, vmem_limit_bytes=VMEM_LIMIT
        ),
        name="train_step",
    )(x, dy, *arrays)


def unpack_kernel(
    w_hbm, g_hbm, mg, mu, md, vg, vu, vd,
    gate, up, down, new_mg, new_mu, new_md, new_vg, new_vu, new_vd,
    held, g_ref, wide, tall, out_wide, out_tall, held_sem, g_sem, load_sem, out_sem, store_sem,
):
    wides, talls = (mg, mu, vg, vu), (md, vd)
    new_wides, new_talls = (new_mg, new_mu, new_vg, new_vu), (new_md, new_vd)

    def load_block(n):
        return pltpu.make_async_copy(w_hbm.at[1 - n // 8, :, n % 2, (n % 8) // 2], held.at[n], held_sem.at[n])

    def load_layer(layer):
        copies = [pltpu.make_async_copy(g_hbm.at[1 - layer], g_ref.at[layer], g_sem.at[layer])]
        for i, ref in enumerate(wides):
            copies.append(pltpu.make_async_copy(ref.at[layer], wide.at[i, layer], load_sem.at[layer, i]))
        for i, ref in enumerate(talls):
            copies.append(pltpu.make_async_copy(ref.at[layer], tall.at[i, layer], load_sem.at[layer, 4 + i]))
        return copies

    def stores(n):
        layer, d, slot = n // 8, n % 8, n % 4
        few, many = pl.ds(pl.multiple_of(d * 96, 32), 96), pl.ds(pl.multiple_of(d * 384, 128), 384)
        return (
            pltpu.make_async_copy(out_wide.at[slot, 0], gate.at[layer, few], out_sem.at[slot, 0]),
            pltpu.make_async_copy(out_wide.at[slot, 1], up.at[layer, few], out_sem.at[slot, 1]),
            pltpu.make_async_copy(out_tall.at[slot], down.at[layer, many], out_sem.at[slot, 2]),
        )

    def moments(g, m_ref, v_ref, at):
        g = g.astype(F32)
        m_ref[at] = 0.9 * m_ref[at] + 0.1 * g
        v_ref[at] = 0.95 * v_ref[at] + 0.05 * g * g

    load_block(0).start()
    load_block(1).start()
    for copy in load_layer(0):
        copy.start()

    @pl.loop(2, 8)
    def _(n):
        load_block(n).start()

    for copy in load_layer(1):
        copy.start()

    @pl.loop(8, 16)
    def _(n):
        load_block(n).start()

    @pl.loop(0, 16)
    def _(n):
        layer, d, slot = n // 8, n % 8, n % 4

        @pl.when(n >= 4)
        def _():
            for copy in stores(n - 4):
                copy.wait()

        load_block(n).wait()
        for j in range(3):
            for half in range(2):
                for i in range(4):
                    to = pl.ds((4 * half + i) * 384 + j * 128, 128)
                    out_wide[slot, 0, :, to] = held[n, 3 * j + half, :96, i * 128 : (i + 1) * 128]
                    out_wide[slot, 1, :, to] = held[n, 3 * j + half, 96:, i * 128 : (i + 1) * 128]
            out_tall[slot, pl.ds(j * 128, 128), :512] = held[n, 3 * j + 2, :128, :]
            out_tall[slot, pl.ds(j * 128, 64), 512:] = held[n, 3 * j + 2, 128:, :256]
            out_tall[slot, pl.ds(j * 128 + 64, 64), 512:] = held[n, 3 * j + 2, 128:, 256:]
        for copy in stores(n):
            copy.start()

        for first in range(2):

            @pl.when(n == 8 * first)
            def _():
                for copy in load_layer(first):
                    copy.wait()

        lanes = pl.ds(pl.multiple_of((d % 4) * 128, 128), 128)
        block = pl.ds(pl.multiple_of(d * 384, 128), 384)
        for mat in range(2):
            for j in range(3):
                at = (layer, slice(None), pl.ds(pl.multiple_of(d * 384 + j * 128, 128), 128))
                g = g_ref[layer, 3 * j + d // 4, 96 * mat : 96 * (mat + 1), lanes]
                moments(g, wide.at[mat], wide.at[2 + mat], at)
        for i, ref in enumerate(new_wides):
            pltpu.make_async_copy(wide.at[i, layer, :, block], ref.at[layer, :, block], store_sem.at[i]).start()

        @pl.when(d < 3)
        def _():
            rows = pl.ds(pl.multiple_of(d * 128, 128), 128)
            for row, count, col, width, to_row, to_col in ((0, 128, 0, 512, 0, 0), (128, 64, 0, 256, 0, 512), (128, 64, 256, 256, 64, 512)):
                g = g_ref[layer, 3 * d + 2, row : row + count, col : col + width]
                at = (layer, pl.ds(pl.multiple_of(d * 128 + to_row, 64), count), slice(to_col, to_col + width))
                moments(g, tall.at[0], tall.at[1], at)
            for i, ref in enumerate(new_talls):
                pltpu.make_async_copy(tall.at[i, layer, rows], ref.at[layer, rows], store_sem.at[4 + i]).start()

    @pl.loop(12, 16)
    def _(n):
        for copy in stores(n):
            copy.wait()

    for i, ref in enumerate(new_wides):
        pltpu.make_async_copy(wide.at[i], ref, store_sem.at[i]).wait()
    for i, ref in enumerate(new_talls):
        pltpu.make_async_copy(tall.at[i], ref, store_sem.at[4 + i]).wait()


def unpack(wout, gout, *moments):
    anywhere = pl.BlockSpec(memory_space=pl.ANY)
    return pl.pallas_call(
        unpack_kernel,
        out_shape=[jax.ShapeDtypeStruct(s, BF) for s in ((2, D, FF), (2, D, FF), (2, FF, D))]
        + [jax.ShapeDtypeStruct(m.shape, F32) for m in moments],
        in_specs=[anywhere] * 8,
        out_specs=[anywhere] * 9,
        scratch_shapes=[
            pltpu.VMEM((16, 9, R, S), BF),
            pltpu.VMEM((2, 9, R, S), BF),
            pltpu.VMEM((4, 2, 96, FF), F32),
            pltpu.VMEM((2, 2, 384, D), F32),
            pltpu.VMEM((4, 2, 96, FF), BF),
            pltpu.VMEM((4, 384, D), BF),
            pltpu.SemaphoreType.DMA((16,)),
            pltpu.SemaphoreType.DMA((2,)),
            pltpu.SemaphoreType.DMA((2, 6)),
            pltpu.SemaphoreType.DMA((4, 3)),
            pltpu.SemaphoreType.DMA((6,)),
        ],
        compiler_params=pltpu.CompilerParams(vmem_limit_bytes=VMEM_LIMIT),
        name="unpack",
    )(wout.reshape(2, 9, 2, 4, R, S), gout.reshape(2, 9, R, S), *moments)


def solution(mesh):
    def body(x, dy, wg, wu, wd, mg, mu, md, vg, vu, vd):
        wout, gout = train_step(x[0], dy[0], wg, wu, wd, mg, mu, md, vg, vu, vd)
        return tuple(unpack(wout, gout, mg, mu, md, vg, vu, vd))

    tok, whole, rows = P(("rep", "dp")), P(), P(None, "dp")
    return jax.shard_map(
        body,
        mesh=mesh,
        in_specs=(tok, tok) + (whole,) * 3 + (rows,) * 6,
        out_specs=(P("rep"),) * 3 + (P("rep", "dp"),) * 6,
        check_vma=False,
    )
```
